256 devices in a mesh: src: 4 (over x), blk: 64 (over y, z, core).
Axes of the slice: x: 4, y: 4, z: 8, core: 2. Of those that a mesh axis runs over, the one named last changes fastest.
Arguments:
- values: float32 [4, 4096, 32, 128], P('src', 'blk'), may hold values from -0.25 to 0.25
- diagonal: float32 [4, 4096, 128], P('src', 'blk'), may hold values from 0.55 to 0.95
- rhs_parts: float32 [4, 4096, 128], P('src', 'blk'), may hold values from -24 to 24
- owner_map: int32 [4096, 128], P('blk'), may hold values from 0 to 3
- columns: int32 [4096, 32, 128], P('blk'), may hold values from 0 to 1073741823
- destination: int32 [4096, 1], P('blk'), may hold values from 0 to 63; in each aligned block of 64 rows (0 to 63, 64 to 127, ...) at most 2 rows name the same one
- order_keys: int32 [4096], P('blk'), may hold values from 0 to 4095, each once
Outputs:
- solution: float32 [4096, 128], P('blk')
The draws below stay inside these ranges and needn't reach their ends.
Inputs may be any that keep to these rules, and one draw needn't show every extreme that they name: `destination`: among the row blocks of one index of blk no owner is named more than 2 times, some owner is named exactly 2 times, and every owner is named by some block. `order_keys`: each key appears once.
All inputs are finite; a program needn't handle non-finite values.
Results may differ from the reference program's by a relative error of at most 0.0003.
Values sent between devices are 32-bit elements; how exact they have to be, the bound alone decides.
A program may use at most 64 MiB of HBM per device.

```python
import math
import jax
import jax.numpy as jnp
import numpy as np
from jax import lax

TD = 64
TR = 128
KOFF = 32
SWEEPS = 3
SEND = 2
TILES = 4096
N_SRC = 4
N_BLK = 64


def with_ends(array, key, low, top_value):
    index_at = [jax.random.randint(jax.random.fold_in(key, axis), (), 0, length) for axis, length in enumerate(array.shape)]
    widest = array.shape.index(max(array.shape))
    beside = index_at[:widest] + [(index_at[widest] + 1) % array.shape[widest]] + index_at[widest + 1:]
    return array.at[tuple(index_at)].set(low).at[tuple(beside)].set(top_value)


def levels(stream_key, dims, shards, least, high):
    def one(dim, shards_of):
        heights = jax.random.uniform(jax.random.fold_in(jax.random.fold_in(stream_key, 6), dim), (shards_of,), jnp.float32, least / len(shards), high / len(shards))
        return jnp.repeat(jnp.exp(heights), dims[dim] // shards_of).reshape((-1,) + (1,) * (len(dims) - dim - 1))

    gain = one(*shards[0])
    for cut in shards[1:]:
        gain = gain * one(*cut)
    return gain


def routed_block(rng, own, number, rows, number_of, top, most, slope):
    order = jax.random.permutation(rng, number_of)
    crowded, usual = shares(number_of, rows * top, most, slope, True), shares(number_of, rows * top, most, slope, False)
    places = jnp.arange(number_of)

    def named(sizes, rotation):
        used = int((sizes > 0).sum())
        fixed = max(1, used // 4)
        moved = fixed + (places - fixed + rotation * (used - fixed)) % max(1, number_of - fixed)
        return jnp.zeros((number_of,), jnp.int32).at[order[jnp.where(places < fixed, places, moved)]].set(jnp.asarray(sizes, jnp.int32))

    sizes = jnp.where(number % 4 == 0, named(crowded, number // 4), named(usual, number - number // 4 - 1))
    mixed = jax.random.permutation(jax.random.fold_in(own, 3), number_of)
    donor, taker = mixed[0:number_of // 2 * 2:2], mixed[1:number_of // 2 * 2:2]
    room = jnp.minimum(sizes[donor] - 1, most - sizes[taker]) // 2
    room = jnp.where((donor == order[0]) | (taker == order[0]) | (sizes[taker] == 0), 0, jnp.maximum(room, 0))
    moved = jax.random.randint(jax.random.fold_in(own, 4), (number_of // 2,), 0, 1 << 20) % (room + 1)
    sizes = sizes.at[donor].add(-moved).at[taker].add(moved)
    members = jnp.searchsorted(jnp.cumsum(sizes), jnp.arange(rows * top), side="right").astype(jnp.int32)
    listing = members.reshape(top, rows).T
    listing = listing[jax.random.permutation(jax.random.fold_in(own, 1), rows)]
    rotation = jax.random.randint(jax.random.fold_in(own, 2), (rows, 1), 0, top)
    return jnp.take_along_axis(listing, (jnp.arange(top)[None, :] + rotation) % top, axis=1)


def shares(number_of, total, most, slope, full):
    loads = [(1 << 20) // math.isqrt(grade ** slope) + 1 for grade in range(1, number_of + 1)]
    largest = most if full else min(most, max(-(-total // number_of), total * loads[0] // sum(loads)))
    least = 1 if total - largest >= number_of - 1 else 0
    given, spare = [largest] + [least] * (number_of - 1), total - largest - least * (number_of - 1)
    while spare > 0:
        free = [i for i in range(1, number_of) if given[i] < largest] or [i for i in range(1, number_of) if given[i] < most]
        whole, budget = sum([loads[i] for i in free]), spare
        for i in free:
            extra = min(most - given[i], max(1, budget * loads[i] // whole), spare)
            given[i] = given[i] + extra
            spare = spare - extra
    return np.array(given)


def gaussian(rng, dims, scale, limit, shards=(), kind=jnp.bfloat16):
    loudness = levels(rng, dims, shards, -0.22, 0.18) if shards else 1.0
    result = jax.random.normal(rng, dims, jnp.float32) * scale * loudness
    return jnp.minimum(jnp.maximum(result, -limit), limit).astype(kind)


def setup_inputs(seed: int = 0) -> dict:
    splits = jax.random.split(jax.random.key(seed), 8)
    values = jnp.clip(jax.random.uniform(splits[0], (N_SRC, TILES, KOFF, TR), jnp.float32, -0.25, 0.25) * levels(splits[0], (N_SRC, TILES, KOFF, TR), ((0, 4), (1, 64)), -0.4, 0.0), -0.25, 0.25)
    diagonal = jnp.clip(0.55 + 0.39999998 * jax.random.uniform(splits[1], (N_SRC, TILES, TR), jnp.float32) ** levels(splits[1], (N_SRC, TILES, TR), ((0, 4), (1, 64)), -0.2, 0.2), 0.55, 0.95)
    rhs_parts = gaussian(splits[2], (N_SRC, TILES, TR), 4.0, 24.0, ((0, 4), (1, 64)), jnp.float32)
    owner_map = with_ends(jax.random.randint(splits[3], (TILES, TR), 0, N_SRC), jax.random.fold_in(splits[3], 1), 0, N_SRC - 1).astype(jnp.int32)
    columns = with_ends(jax.random.randint(splits[4], (TILES, KOFF, TR), 0, 1073741824), jax.random.fold_in(splits[4], 1), 0, 1073741823).astype(jnp.int32)
    destination_keys = jax.random.split(jax.random.fold_in(splits[5], 1), TILES // TD)
    destination_turns = jax.random.permutation(jax.random.fold_in(splits[5], 3), TILES // TD)
    destination = jax.vmap(lambda own, number: routed_block(jax.random.fold_in(splits[5], 2), own, number, TD, N_BLK, 1, SEND, 2))(destination_keys, destination_turns).reshape((TILES, 1))
    order_keys = jax.random.permutation(splits[6], TILES).astype(jnp.int32)
    return dict(values=values, diagonal=diagonal, rhs_parts=rhs_parts, owner_map=owner_map, columns=columns, destination=destination, order_keys=order_keys)


def reference(values, diagonal, rhs_parts, owner_map, columns, destination, order_keys):
    owner_of = destination[:, 0]
    same_owner = owner_of[:, None] == owner_of[None, :]
    tile_rank = jnp.sum(same_owner & (order_keys[None, :] < order_keys[:, None]), axis=1).astype(jnp.int32)
    owner_ids = jnp.arange(N_BLK, dtype=jnp.int32)
    owner_counts = jnp.sum(owner_of[None, :] == owner_ids[:, None], axis=1).astype(jnp.int32)
    slot_count = N_BLK * SEND
    slot_table = jnp.full((N_BLK, slot_count), -1, jnp.int32)
    slot_table = slot_table.at[owner_of, tile_rank].set(jnp.arange(TILES, dtype=jnp.int32))
    assembled = jnp.sum(values, axis=0)
    assembled_diag = jnp.sum(diagonal, axis=0)
    right_side = jnp.take_along_axis(rhs_parts, owner_map[None, :, :], axis=0)[0]
    slot_numbers = jnp.arange(slot_count, dtype=jnp.int32)

    def solve_owner(owner):
        chosen = slot_table[owner]
        is_live = chosen >= 0
        safe_index = jnp.maximum(chosen, 0)
        block_vals = jnp.where(is_live[:, None, None], assembled[safe_index], 0.0)
        block_cols = columns[safe_index]
        block_right = jnp.where(is_live[:, None], right_side[safe_index], 0.0)
        block_diag = jnp.where(is_live[:, None], assembled_diag[safe_index], 1.0)
        step_over = jnp.remainder(block_cols // TR, 2).astype(jnp.int32)
        target_tile = jnp.remainder(slot_numbers[:, None, None] + step_over, owner_counts[owner]).astype(jnp.int32)
        location = (target_tile * TR + jnp.remainder(block_cols, TR)).astype(jnp.int32)
        iterate = jnp.zeros((slot_count * TR,), jnp.float32)
        for sweep_index in range(SWEEPS):
            nearby = iterate[location]
            summed = jnp.sum(block_vals * nearby, axis=1)
            update = jnp.where(is_live[:, None], (block_right - summed) / block_diag, 0.0)
            iterate = update.reshape(-1)
        return iterate.reshape(slot_count, TR)

    solved = lax.map(solve_owner, owner_ids)
    return solved[owner_of, tile_rank]
```

```python
import functools

import jax
import jax.numpy as jnp
from jax import lax
from jax.experimental import pallas as pl
from jax.experimental.pallas import tpu as pltpu
from jax.sharding import PartitionSpec as P

SWEEPS = 3
EXACT = lax.Precision.HIGHEST


def pick(selector, table):
    return jnp.dot(selector, table, precision=EXACT, preferred_element_type=jnp.float32)


def iota(shape, dim):
    return lax.broadcasted_iota(jnp.int32, shape, dim)


def turned(row, size):
    square = jnp.where(iota((size, size), 0) == iota((size, size), 1), row, 0.0)
    return jnp.sum(square, axis=1, keepdims=True)


def source_slots(owner_row, tiles, slots):
    owner_col = turned(owner_row, tiles)
    same = owner_col == owner_row
    row_at, col_at = iota((tiles, tiles), 0), iota((tiles, tiles), 1)
    before_col = jnp.sum(jnp.where(same & (col_at < row_at), 1.0, 0.0), axis=1, keepdims=True)
    before_row = jnp.sum(jnp.where(same & (row_at < col_at), 1.0, 0.0), axis=0, keepdims=True)
    slot_col = 2.0 * owner_col + before_col
    slot_row = 2.0 * owner_row + before_row
    to_slots = jnp.where(iota((slots, tiles), 0).astype(jnp.float32) == slot_row, 1.0, 0.0)
    from_slots = jnp.where(iota((tiles, slots), 1).astype(jnp.float32) == slot_col, 1.0, 0.0)
    return to_slots, from_slots


def successor(owners, keys, me, tiles, key_count):
    peers, width = owners.shape
    slots = 2 * peers
    lane = iota((peers, width), 1).astype(jnp.float32)
    mine = (owners == me.astype(jnp.float32)) & (lane < tiles)
    first = jnp.min(jnp.where(mine, lane, 1e6), axis=1, keepdims=True)
    last = jnp.max(jnp.where(mine, lane, -1.0), axis=1, keepdims=True)
    key_first = jnp.sum(jnp.where(mine & (lane == first), keys, 0.0), axis=1, keepdims=True)
    key_last = jnp.sum(jnp.where(mine & (lane == last), keys, 0.0), axis=1, keepdims=True)
    key_first = jnp.where(last >= 0.0, key_first, -1.0)
    key_last = jnp.where(last > first, key_last, -1.0)
    slot = iota((peers, slots), 1)
    chosen = jnp.where(slot % 2 == 1, key_last, key_first)
    key_row = jnp.sum(jnp.where(slot // 2 == iota((peers, slots), 0), chosen, 0.0), axis=0, keepdims=True)
    ahead = key_row - turned(key_row, slots) - 1.0
    ahead = jnp.where(ahead < 0.0, ahead + key_count, ahead)
    ahead = jnp.where(key_row >= 0.0, ahead, 4.0 * key_count)
    nearest = jnp.min(ahead, axis=1, keepdims=True)
    return jnp.where(ahead == nearest, 1.0, 0.0)


def kernel(
    n_src, n_blk, tiles, stored, rows, key_count,
    vals_in, cols_in, diag_in, rhs_in, map_in, dest_in, keys_in, out,
    vals, cols, diag, rhs, owner_map, dest, keys,
    meta_own, meta_all, shares, slot_out, slot_in, next_out, next_in, prods,
    here, there, fixed, load_sem, meta_sem, share_sem, slot_sem, next_sem, prod_sem,
):
    src, blk = lax.axis_index("src"), lax.axis_index("blk")
    slots = 2 * n_blk

    barrier = pltpu.get_barrier_semaphore()

    @pl.loop(1, n_blk)
    def _(step):
        pl.semaphore_signal(barrier, 1, device_id={"blk": lax.rem(blk + step, n_blk)})

    for step in range(1, n_src):
        pl.semaphore_signal(barrier, 1, device_id={"src": lax.rem(src + step, n_src)})

    loads = [
        pltpu.make_async_copy(a, b, load_sem.at[k])
        for k, (a, b) in enumerate((
            (dest_in, dest), (keys_in, keys), (map_in, owner_map), (rhs_in.at[0], rhs),
            (diag_in.at[0], diag), (cols_in, cols), (vals_in.at[0], vals)))
    ]
    for load in loads:
        load.start()
    loads[0].wait()
    loads[1].wait()
    meta_own[...] = jnp.zeros_like(meta_own)
    meta_own[0:1, 0:tiles] = dest[...]
    meta_own[1:2, 0:tiles] = keys[...]
    meta_all[blk] = meta_own[...]
    to_slots, from_slots = source_slots(dest[...].astype(jnp.float32), tiles, slots)
    for load in loads[2:5]:
        load.wait()
    shares[src, 0] = jnp.where(owner_map[...] == src, rhs[...], 0.0)
    shares[src, 1] = diag[...]
    pl.semaphore_wait(barrier, n_blk - 1 + n_src - 1)

    def to_src(buffer, sem):
        copies = []
        for step in range(1, n_src):
            copies.append(pltpu.make_async_remote_copy(
                src_ref=buffer.at[src], dst_ref=buffer.at[src],
                send_sem=sem.at[0, step], recv_sem=sem.at[1, step],
                device_id={"src": lax.rem(src + step, n_src)}))
        for copy in copies:
            copy.start()
        return copies

    def to_blk(source, target, sem):
        @pl.loop(1, n_blk)
        def _(step):
            peer = lax.rem(blk + step, n_blk)
            pltpu.make_async_remote_copy(
                src_ref=source.at[peer], dst_ref=target.at[blk],
                send_sem=sem.at[0], recv_sem=sem.at[1], device_id={"blk": peer}).start()
        target[blk] = source[blk]

    def all_of(buffer, sem):
        most = buffer.at[pl.ds(0, n_blk - 1)]
        pltpu.make_async_copy(most, most, sem).wait()

    share_copies = to_src(shares, share_sem)

    @pl.loop(1, n_blk)
    def _(step):
        peer = lax.rem(blk + step, n_blk)
        pltpu.make_async_remote_copy(
            src_ref=meta_own, dst_ref=meta_all.at[blk],
            send_sem=meta_sem.at[0], recv_sem=meta_sem.at[1], device_id={"blk": peer}).start()

    for copy in share_copies:
        copy.wait()
    fixed[0] = functools.reduce(jnp.add, [shares[s, 0] for s in range(n_src)])
    fixed[1] = functools.reduce(jnp.add, [shares[s, 1] for s in range(n_src)])
    here[...] = fixed[0] / fixed[1]

    for sweep in range(1, SWEEPS):
        e = sweep - 1
        slot_out[e] = pick(to_slots, here[...]).reshape(n_blk, 2, rows)
        to_blk(slot_out.at[e], slot_in.at[e], slot_sem.at[e])
        if e == 0:
            all_of(meta_all, meta_sem.at[1])
            follow = successor(
                meta_all[:, 0, :].astype(jnp.float32), meta_all[:, 1, :].astype(jnp.float32), blk, tiles, key_count)
        all_of(slot_in.at[e], slot_sem.at[e, 1])
        next_out[e] = pick(follow, slot_in[e].reshape(slots, rows)).reshape(n_blk, 2, rows)
        to_blk(next_out.at[e], next_in.at[e], next_sem.at[e])
        all_of(next_in.at[e], next_sem.at[e, 1])
        there[...] = pick(from_slots, next_in[e].reshape(slots, rows))
        if e == 0:
            loads[5].wait()
            loads[6].wait()

        @pl.loop(0, tiles // 8)
        def _(group):
            base = group * 8
            lines = []
            for k in range(8):
                code = cols[base + k]
                lane = code & (rows - 1)
                own = jnp.broadcast_to(here[pl.ds(base + k, 1), :], (stored, rows))
                nxt = jnp.broadcast_to(there[pl.ds(base + k, 1), :], (stored, rows))
                near = jnp.where(
                    (code & rows) == 0,
                    jnp.take_along_axis(own, lane, axis=1),
                    jnp.take_along_axis(nxt, lane, axis=1))
                lines.append(jnp.sum(vals[base + k] * near, axis=0, keepdims=True))
            prods[e, src, pl.ds(pl.multiple_of(base, 8), 8), :] = jnp.concatenate(lines, axis=0)

        prod_copies = to_src(prods.at[e], prod_sem.at[e])
        for copy in prod_copies:
            copy.wait()
        total = functools.reduce(jnp.add, [prods[e, s] for s in range(n_src)])
        here[...] = (fixed[0] - total) / fixed[1]
    out[...] = here[...]

    all_of(meta_all, meta_sem.at[0])
    for e in range(SWEEPS - 1):
        all_of(slot_out.at[e], slot_sem.at[e, 0])
        all_of(next_out.at[e], next_sem.at[e, 0])


def solution(mesh):
    n_src, n_blk = mesh.shape["src"], mesh.shape["blk"]

    def on_device(values, diagonal, rhs_parts, owner_map, columns, destination, order_keys):
        tiles, stored, rows = columns.shape
        key_count = float(tiles * n_blk)
        row = jnp.float32
        anywhere = pl.BlockSpec(memory_space=pl.ANY)
        steps = SWEEPS - 1
        dma = pltpu.SemaphoreType.DMA
        return pl.pallas_call(
            functools.partial(kernel, n_src, n_blk, tiles, stored, rows, key_count),
            out_shape=jax.ShapeDtypeStruct((tiles, rows), row),
            in_specs=[anywhere] * 7,
            out_specs=pl.BlockSpec(memory_space=pltpu.VMEM),
            scratch_shapes=[
                pltpu.VMEM((tiles, stored, rows), row),
                pltpu.VMEM((tiles, stored, rows), jnp.int32),
                pltpu.VMEM((tiles, rows), row),
                pltpu.VMEM((tiles, rows), row),
                pltpu.VMEM((tiles, rows), jnp.int32),
                pltpu.VMEM((1, tiles), jnp.int32),
                pltpu.VMEM((1, tiles), jnp.int32),
                pltpu.VMEM((2, rows), jnp.int32),
                pltpu.VMEM((n_blk, 2, rows), jnp.int32),
                pltpu.VMEM((n_src, 2, tiles, rows), row),
                pltpu.VMEM((steps, n_blk, 2, rows), row),
                pltpu.VMEM((steps, n_blk, 2, rows), row),
                pltpu.VMEM((steps, n_blk, 2, rows), row),
                pltpu.VMEM((steps, n_blk, 2, rows), row),
                pltpu.VMEM((steps, n_src, tiles, rows), row),
                pltpu.VMEM((tiles, rows), row),
                pltpu.VMEM((tiles, rows), row),
                pltpu.VMEM((2, tiles, rows), row),
                dma((7,)),
                dma((2,)),
                dma((2, n_src)),
                dma((steps, 2)),
                dma((steps, 2)),
                dma((steps, 2, n_src)),
            ],
            compiler_params=pltpu.CompilerParams(collective_id=0, has_side_effects=True),
            name="sweeps",
        )(values, columns, diagonal, rhs_parts, owner_map,
          destination.reshape(1, tiles), order_keys.reshape(1, tiles))

    placed = (
        P("src", "blk", None, None), P("src", "blk", None), P("src", "blk", None),
        P("blk", None), P("blk", None, None), P("blk", None), P("blk"),
    )
    return jax.shard_map(
        on_device, mesh=mesh, in_specs=placed, out_specs=P("blk", None), check_vma=False)
```

```python
import functools

import jax
import jax.numpy as jnp
from jax import lax
from jax.experimental import pallas as pl
from jax.experimental.pallas import tpu as pltpu
from jax.sharding import PartitionSpec as P

SWEEPS = 3
EXACT = lax.Precision.HIGHEST


def pick(selector, table):
    return jnp.dot(selector, table, precision=EXACT, preferred_element_type=jnp.float32)


def iota(shape, dim):
    return lax.broadcasted_iota(jnp.int32, shape, dim)


def turned(row, size):
    square = jnp.where(iota((size, size), 0) == iota((size, size), 1), row, 0.0)
    return jnp.sum(square, axis=1, keepdims=True)


def source_slots(owner_row, tiles, slots):
    owner_col = turned(owner_row, tiles)
    same = owner_col == owner_row
    row_at, col_at = iota((tiles, tiles), 0), iota((tiles, tiles), 1)
    before_col = jnp.sum(jnp.where(same & (col_at < row_at), 1.0, 0.0), axis=1, keepdims=True)
    before_row = jnp.sum(jnp.where(same & (row_at < col_at), 1.0, 0.0), axis=0, keepdims=True)
    slot_col = 2.0 * owner_col + before_col
    slot_row = 2.0 * owner_row + before_row
    to_slots = jnp.where(iota((slots, tiles), 0).astype(jnp.float32) == slot_row, 1.0, 0.0)
    from_slots = jnp.where(iota((tiles, slots), 1).astype(jnp.float32) == slot_col, 1.0, 0.0)
    return to_slots, from_slots


def successor(owners, keys, me, tiles, key_count):
    peers, width = owners.shape
    slots = 2 * peers
    lane = iota((peers, width), 1).astype(jnp.float32)
    mine = (owners == me.astype(jnp.float32)) & (lane < tiles)
    first = jnp.min(jnp.where(mine, lane, 1e6), axis=1, keepdims=True)
    last = jnp.max(jnp.where(mine, lane, -1.0), axis=1, keepdims=True)
    key_first = jnp.sum(jnp.where(mine & (lane == first), keys, 0.0), axis=1, keepdims=True)
    key_last = jnp.sum(jnp.where(mine & (lane == last), keys, 0.0), axis=1, keepdims=True)
    key_first = jnp.where(last >= 0.0, key_first, -1.0)
    key_last = jnp.where(last > first, key_last, -1.0)
    slot = iota((peers, slots), 1)
    chosen = jnp.where(slot % 2 == 1, key_last, key_first)
    key_row = jnp.sum(jnp.where(slot // 2 == iota((peers, slots), 0), chosen, 0.0), axis=0, keepdims=True)
    ahead = key_row - turned(key_row, slots) - 1.0
    ahead = jnp.where(ahead < 0.0, ahead + key_count, ahead)
    ahead = jnp.where(key_row >= 0.0, ahead, 4.0 * key_count)
    nearest = jnp.min(ahead, axis=1, keepdims=True)
    return jnp.where(ahead == nearest, 1.0, 0.0)


def folded(parts):
    parts = [parts[k] for k in (0, 4, 2, 6, 1, 5, 3, 7)]
    line = iota(parts[0].shape, 0)
    for step in (1, 2, 4):
        half = len(parts) // 2
        low = (line & step) == 0
        parts = [
            jnp.where(low, parts[k], parts[k + half])
            + pltpu.roll(jnp.where(low, parts[k + half], parts[k]), step, 0)
            for k in range(half)
        ]
    return parts[0]


def products(vals, cols, lines, v0, t0, bit):
    _, stored, rows = cols.shape
    parts = []
    for k in range(8):
        line = jnp.broadcast_to(lines[pl.ds(t0 + k, 1), :], (8, rows))
        total = None
        for j in range(stored // 8):
            code = cols[t0 + k, pl.ds(8 * j, 8), :]
            near = jnp.take_along_axis(line, code & (rows - 1), axis=1, mode="promise_in_bounds")
            term = jnp.where((code & rows) == bit, vals[v0 + k, pl.ds(8 * j, 8), :], 0.0) * near
            total = term if total is None else total + term
        parts.append(total)
    return folded(parts)


def kernel(
    n_src, n_blk, grid, tiles, stored, rows, key_count,
    vals_in, cols_in, diag_in, rhs_in, map_in, dest_in, keys_in, out,
    vals, cols, diag, rhs, owner_map, dest, keys,
    meta_own, meta_all, shares, slot_out, slot_in, next_out, next_in,
    parts, full, quarters, here, there, near, fixed,
    load_sem, meta_sem, share_sem, slot_sem, next_sem, part_sem, full_sem, quarter_sem,
):
    src, blk = lax.axis_index("src"), lax.axis_index("blk")
    slots = 2 * n_blk
    share = tiles // n_src
    n_y, n_z = grid
    y, z, core = blk // (2 * n_z), (blk // 2) % n_z, blk % 2
    src_steps = sorted(range(1, n_src), key=lambda step: -min(step, n_src - step))

    barrier = pltpu.get_barrier_semaphore()

    @pl.loop(1, n_blk)
    def _(step):
        pl.semaphore_signal(barrier, 1, device_id={"blk": lax.rem(blk + step, n_blk)})

    for step in src_steps:
        pl.semaphore_signal(barrier, 1, device_id={"src": lax.rem(src + step, n_src)})

    mine = pl.ds(pl.multiple_of(src * share, share), share)
    loads = [
        pltpu.make_async_copy(a, b, load_sem.at[k])
        for k, (a, b) in enumerate((
            (dest_in, dest), (keys_in, keys), (map_in, owner_map), (rhs_in.at[0], rhs),
            (diag_in.at[0], diag), (vals_in.at[0], vals), (vals_in.at[0, mine], parts.at[src]),
            (cols_in, cols)))
    ]
    for load in loads:
        load.start()
    loads[0].wait()
    loads[1].wait()
    meta_own[...] = jnp.zeros_like(meta_own)
    meta_own[0:1, 0:tiles] = dest[...]
    meta_own[1:2, 0:tiles] = keys[...]
    meta_all[blk] = meta_own[...]
    to_slots, from_slots = source_slots(dest[...].astype(jnp.float32), tiles, slots)
    for load in loads[2:5]:
        load.wait()
    shares[src, 0] = jnp.where(owner_map[...] == src, rhs[...], 0.0)
    shares[src, 1] = diag[...]
    for load in loads[5:]:
        load.wait()
    pl.semaphore_wait(barrier, n_blk - 1 + n_src - 1)

    def to_src(source, target, sem):
        copies = []
        for step in src_steps:
            peer = lax.rem(src + step, n_src)
            copies.append(pltpu.make_async_remote_copy(
                src_ref=source(peer), dst_ref=target, send_sem=sem.at[0, step],
                recv_sem=sem.at[1, step], device_id={"src": peer}))
        for copy in copies:
            copy.start()
        return copies

    def to_blk(source, target, sem):
        @pl.loop(0, n_blk - 1)
        def _(step):
            turn_z, turn_y, turn_c = step // (2 * n_y), (step // 2) % n_y, step % 2
            to_z = n_z // 2 + (turn_z % 2) * -(turn_z // 2 + 1) + (1 - turn_z % 2) * (turn_z // 2)
            to_y = n_y // 2 + (turn_y % 2) * -(turn_y // 2 + 1) + (1 - turn_y % 2) * (turn_y // 2)
            peer = (((y + to_y) % n_y) * n_z + (z + to_z) % n_z) * 2 + (core + 1 + turn_c) % 2
            pltpu.make_async_remote_copy(
                src_ref=source(peer), dst_ref=target.at[blk],
                send_sem=sem.at[0], recv_sem=sem.at[1], device_id={"blk": peer}).start()

    def all_of(buffer, sem):
        most = buffer.at[pl.ds(0, n_blk - 1)]
        pltpu.make_async_copy(most, most, sem).wait()

    def through_owners(e, lines, follow):
        slot_out[e] = pick(to_slots, lines).reshape(n_blk, 2, rows)
        to_blk(lambda peer: slot_out.at[e, peer], slot_in.at[e], slot_sem.at[e])
        slot_in[e, blk] = slot_out[e, blk]
        if follow is None:
            all_of(meta_all, meta_sem.at[1])
            follow = successor(
                meta_all[:, 0, :].astype(jnp.float32), meta_all[:, 1, :].astype(jnp.float32),
                blk, tiles, key_count)
        all_of(slot_in.at[e], slot_sem.at[e, 1])
        next_out[e] = pick(follow, slot_in[e].reshape(slots, rows)).reshape(n_blk, 2, rows)
        to_blk(lambda peer: next_out.at[e, peer], next_in.at[e], next_sem.at[e])
        next_in[e, blk] = next_out[e, blk]
        return follow

    def from_owners(e):
        all_of(next_in.at[e], next_sem.at[e, 1])
        there[...] = pick(from_slots, next_in[e].reshape(slots, rows))

    share_copies = to_src(lambda peer: shares.at[src], shares.at[src], share_sem)
    to_blk(lambda peer: meta_own, meta_all, meta_sem)
    part_copies = to_src(
        lambda peer: vals.at[pl.ds(pl.multiple_of(peer * share, share), share)], parts.at[src], part_sem)
    for copy in share_copies:
        copy.wait()
    fixed[0] = functools.reduce(jnp.add, [shares[s, 0] for s in range(n_src)])
    fixed[1] = functools.reduce(jnp.add, [shares[s, 1] for s in range(n_src)])
    here[...] = fixed[0] / fixed[1]
    follow = through_owners(0, here[...], None)

    for copy in part_copies:
        copy.wait()

    @pl.loop(0, share)
    def _(k):
        full[src, k] = functools.reduce(jnp.add, [parts[s, k] for s in range(n_src)])

    first = pl.multiple_of(src * share, share)

    @pl.loop(0, share // 8)
    def _(g):
        near[pl.ds(pl.multiple_of(first + g * 8, 8), 8), :] = products(
            full.at[src], cols, here, g * 8, first + g * 8, 0)

    from_owners(0)
    for g in range(share // 8):
        at = pl.ds(pl.multiple_of(first + g * 8, 8), 8)
        total = near[at, :] + products(full.at[src], cols, there, g * 8, first + g * 8, rows)
        quarters[src, pl.ds(g * 8, 8), :] = (fixed[0, at, :] - total) / fixed[1, at, :]
    quarter_copies = to_src(lambda peer: quarters.at[src], quarters.at[src], quarter_sem)
    full_copies = to_src(lambda peer: full.at[src], full.at[src], full_sem)
    for copy in quarter_copies:
        copy.wait()
    here[...] = quarters[...].reshape(tiles, rows)
    through_owners(1, here[...], follow)

    def near_of(s):
        @pl.loop(0, share // 8)
        def _(g):
            start = s * share + g * 8
            near[pl.ds(pl.multiple_of(start, 8), 8), :] = products(full.at[s], cols, here, g * 8, start, 0)

    near_of(src)
    for step, copy in sorted(zip(src_steps, full_copies), key=lambda pair: min(pair[0], n_src - pair[0])):
        copy.wait()
        near_of(lax.rem(src - step + n_src, n_src))
    from_owners(1)
    for s in range(n_src):
        for g in range(share // 8):
            at = pl.ds(s * share + g * 8, 8)
            total = near[at, :] + products(full.at[s], cols, there, g * 8, s * share + g * 8, rows)
            out[at, :] = (fixed[0, at, :] - total) / fixed[1, at, :]

    all_of(meta_all, meta_sem.at[0])
    for e in range(SWEEPS - 1):
        all_of(slot_out.at[e], slot_sem.at[e, 0])
        all_of(next_out.at[e], next_sem.at[e, 0])


def solution(mesh):
    n_src, n_blk = mesh.shape["src"], mesh.shape["blk"]
    grid = (4, n_blk // 8)

    def on_device(values, diagonal, rhs_parts, owner_map, columns, destination, order_keys):
        tiles, stored, rows = columns.shape
        key_count = float(tiles * n_blk)
        row = jnp.float32
        anywhere = pl.BlockSpec(memory_space=pl.ANY)
        steps = SWEEPS - 1
        dma = pltpu.SemaphoreType.DMA
        return pl.pallas_call(
            functools.partial(kernel, n_src, n_blk, grid, tiles, stored, rows, key_count),
            out_shape=jax.ShapeDtypeStruct((tiles, rows), row),
            in_specs=[anywhere] * 7,
            out_specs=pl.BlockSpec(memory_space=pltpu.VMEM),
            scratch_shapes=[
                pltpu.VMEM((tiles, stored, rows), row),
                pltpu.VMEM((tiles, stored, rows), jnp.int32),
                pltpu.VMEM((tiles, rows), row),
                pltpu.VMEM((tiles, rows), row),
                pltpu.VMEM((tiles, rows), jnp.int32),
                pltpu.VMEM((1, tiles), jnp.int32),
                pltpu.VMEM((1, tiles), jnp.int32),
                pltpu.VMEM((2, rows), jnp.int32),
                pltpu.VMEM((n_blk, 2, rows), jnp.int32),
                pltpu.VMEM((n_src, 2, tiles, rows), row),
                pltpu.VMEM((steps, n_blk, 2, rows), row),
                pltpu.VMEM((steps, n_blk, 2, rows), row),
                pltpu.VMEM((steps, n_blk, 2, rows), row),
                pltpu.VMEM((steps, n_blk, 2, rows), row),
                pltpu.VMEM((n_src, tiles // n_src, stored, rows), row),
                pltpu.VMEM((n_src, tiles // n_src, stored, rows), row),
                pltpu.VMEM((n_src, tiles // n_src, rows), row),
                pltpu.VMEM((tiles, rows), row),
                pltpu.VMEM((tiles, rows), row),
                pltpu.VMEM((tiles, rows), row),
                pltpu.VMEM((2, tiles, rows), row),
                dma((8,)),
                dma((2,)),
                dma((2, n_src)),
                dma((steps, 2)),
                dma((steps, 2)),
                dma((2, n_src)),
                dma((2, n_src)),
                dma((2, n_src)),
            ],
            compiler_params=pltpu.CompilerParams(collective_id=0, has_side_effects=True),
            name="sweeps",
        )(values, columns, diagonal, rhs_parts, owner_map,
          destination.reshape(1, tiles), order_keys.reshape(1, tiles))

    placed = (
        P("src", "blk", None, None), P("src", "blk", None), P("src", "blk", None),
        P("blk", None), P("blk", None, None), P("blk", None), P("blk"),
    )
    return jax.shard_map(
        on_device, mesh=mesh, in_specs=placed, out_specs=P("blk", None), check_vma=False)
```

```python
import functools

import jax
import jax.numpy as jnp
from jax import lax
from jax.experimental import pallas as pl
from jax.experimental.pallas import tpu as pltpu
from jax.sharding import PartitionSpec as P

SWEEPS = 3
EXACT = lax.Precision.HIGHEST


def pick(selector, table):
    return jnp.dot(selector, table, precision=EXACT, preferred_element_type=jnp.float32)


def iota(shape, dim):
    return lax.broadcasted_iota(jnp.int32, shape, dim)


def turned(row, size):
    square = jnp.where(iota((size, size), 0) == iota((size, size), 1), row, 0.0)
    return jnp.sum(square, axis=1, keepdims=True)


def source_slots(owner_row, tiles, slots):
    owner_col = turned(owner_row, tiles)
    same = owner_col == owner_row
    row_at, col_at = iota((tiles, tiles), 0), iota((tiles, tiles), 1)
    before_col = jnp.sum(jnp.where(same & (col_at < row_at), 1.0, 0.0), axis=1, keepdims=True)
    before_row = jnp.sum(jnp.where(same & (row_at < col_at), 1.0, 0.0), axis=0, keepdims=True)
    slot_col = 2.0 * owner_col + before_col
    slot_row = 2.0 * owner_row + before_row
    to_slots = jnp.where(iota((slots, tiles), 0).astype(jnp.float32) == slot_row, 1.0, 0.0)
    from_slots = jnp.where(iota((tiles, slots), 1).astype(jnp.float32) == slot_col, 1.0, 0.0)
    return to_slots, from_slots


def successor(owners, keys, me, tiles, key_count):
    peers, width = owners.shape
    slots = 2 * peers
    lane = iota((peers, width), 1).astype(jnp.float32)
    mine = (owners == me.astype(jnp.float32)) & (lane < tiles)
    first = jnp.min(jnp.where(mine, lane, 1e6), axis=1, keepdims=True)
    last = jnp.max(jnp.where(mine, lane, -1.0), axis=1, keepdims=True)
    key_first = jnp.sum(jnp.where(mine & (lane == first), keys, 0.0), axis=1, keepdims=True)
    key_last = jnp.sum(jnp.where(mine & (lane == last), keys, 0.0), axis=1, keepdims=True)
    key_first = jnp.where(last >= 0.0, key_first, -1.0)
    key_last = jnp.where(last > first, key_last, -1.0)
    slot = iota((peers, slots), 1)
    chosen = jnp.where(slot % 2 == 1, key_last, key_first)
    key_row = jnp.sum(jnp.where(slot // 2 == iota((peers, slots), 0), chosen, 0.0), axis=0, keepdims=True)
    ahead = key_row - turned(key_row, slots) - 1.0
    ahead = jnp.where(ahead < 0.0, ahead + key_count, ahead)
    ahead = jnp.where(key_row >= 0.0, ahead, 4.0 * key_count)
    nearest = jnp.min(ahead, axis=1, keepdims=True)
    return jnp.where(ahead == nearest, 1.0, 0.0)


def folded(parts):
    parts = [parts[k] for k in (0, 4, 2, 6, 1, 5, 3, 7)]
    line = iota(parts[0].shape, 0)
    for step in (1, 2, 4):
        half = len(parts) // 2
        low = (line & step) == 0
        parts = [
            jnp.where(low, parts[k], parts[k + half])
            + pltpu.roll(jnp.where(low, parts[k + half], parts[k]), step, 0)
            for k in range(half)
        ]
    return parts[0]


def products(vals, cols, lines, v0, t0, bit):
    _, stored, rows = cols.shape
    parts = []
    for k in range(8):
        line = jnp.broadcast_to(lines[pl.ds(t0 + k, 1), :], (8, rows))
        total = None
        for j in range(stored // 8):
            code = cols[t0 + k, pl.ds(8 * j, 8), :]
            near = jnp.take_along_axis(line, code & (rows - 1), axis=1, mode="promise_in_bounds")
            term = jnp.where((code & rows) == bit, vals[v0 + k, pl.ds(8 * j, 8), :], 0.0) * near
            total = term if total is None else total + term
        parts.append(total)
    return folded(parts)


def kernel(
    n_src, n_blk, grid, tiles, stored, rows, key_count,
    vals_in, cols_in, diag_in, rhs_in, map_in, dest_in, keys_in, out,
    vals, cols, diag, rhs, owner_map, dest, keys,
    meta_own, meta_all, shares, slot_out, slot_in, next_out, next_in,
    parts, full, quarters, here, there, near, fixed,
    load_sem, meta_sem, share_sem, slot_sem, next_sem, part_sem, full_sem, quarter_sem, group_sem, open_sem,
):
    src, blk = lax.axis_index("src"), lax.axis_index("blk")
    slots = 2 * n_blk
    share = tiles // n_src
    n_y, n_z = grid
    y, z, core = blk // (2 * n_z), (blk // 2) % n_z, blk % 2
    src_steps = sorted(range(1, n_src), key=lambda step: -min(step, n_src - step))

    def far_first(step):
        turn_z, turn_y, turn_c = step // (2 * n_y), (step // 2) % n_y, step % 2
        to_z = n_z // 2 + (turn_z % 2) * -(turn_z // 2 + 1) + (1 - turn_z % 2) * (turn_z // 2)
        to_y = n_y // 2 + (turn_y % 2) * -(turn_y // 2 + 1) + (1 - turn_y % 2) * (turn_y // 2)
        return (((y + to_y) % n_y) * n_z + (z + to_z) % n_z) * 2 + (core + 1 + turn_c) % 2

    barrier = pltpu.get_barrier_semaphore()
    leader = n_src - 1
    for step in src_steps:
        peer = lax.rem(src + step, n_src)

        @pl.when(peer != leader)
        def _():
            pl.semaphore_signal(barrier, 1, device_id={"src": peer})

    mine = pl.ds(pl.multiple_of(src * share, share), share)
    loads = [
        pltpu.make_async_copy(a, b, load_sem.at[k])
        for k, (a, b) in enumerate((
            (dest_in, dest), (keys_in, keys), (map_in, owner_map), (rhs_in.at[0], rhs),
            (diag_in.at[0], diag), (vals_in.at[0], vals), (vals_in.at[0, mine], parts.at[src]),
            (cols_in, cols)))
    ]
    for load in loads:
        load.start()
    loads[0].wait()
    loads[1].wait()
    meta_own[...] = jnp.zeros_like(meta_own)
    meta_own[0:1, 0:tiles] = dest[...]
    meta_own[1:2, 0:tiles] = keys[...]
    meta_all[blk] = meta_own[...]
    to_slots, from_slots = source_slots(dest[...].astype(jnp.float32), tiles, slots)
    for load in loads[2:5]:
        load.wait()
    shares[src, 0] = jnp.where(owner_map[...] == src, rhs[...], 0.0)
    shares[src, 1] = diag[...]
    for load in loads[5:]:
        load.wait()

    @pl.when(src != leader)
    def _():
        pl.semaphore_wait(barrier, n_src - 1)
        pl.semaphore_signal(group_sem, 1, device_id={"src": leader})

    @pl.when(src == leader)
    def _():
        pl.semaphore_wait(group_sem, n_src - 1)

        @pl.loop(0, n_blk - 1)
        def _(step):
            pl.semaphore_signal(barrier, 1, device_id={"blk": far_first(step)})

    def to_src(source, target, sem):
        copies = []
        for step in src_steps:
            peer = lax.rem(src + step, n_src)
            copies.append(pltpu.make_async_remote_copy(
                src_ref=source(peer), dst_ref=target, send_sem=sem.at[0, step],
                recv_sem=sem.at[1, step], device_id={"src": peer}))
        for copy in copies:
            copy.start()
        return copies

    def to_blk(source, target, sem):
        @pl.loop(0, n_blk - 1)
        def _(step):
            peer = far_first(step)
            pltpu.make_async_remote_copy(
                src_ref=source(peer), dst_ref=target.at[blk],
                send_sem=sem.at[0], recv_sem=sem.at[1], device_id={"blk": peer}).start()

    def ring_copy(chunk, part, step, k):
        block = full.at[chunk, part] if part is not None else full.at[chunk]
        return pltpu.make_async_remote_copy(
            src_ref=block, dst_ref=block, send_sem=full_sem.at[0, k], recv_sem=full_sem.at[1, k],
            device_id={"src": (src + step) % n_src})

    def all_of(buffer, sem):
        most = buffer.at[pl.ds(0, n_blk - 1)]
        pltpu.make_async_copy(most, most, sem).wait()

    def through_owners(e, lines, follow, meanwhile=lambda: None):
        slot_out[e] = pick(to_slots, lines).reshape(n_blk, 2, rows)
        to_blk(lambda peer: slot_out.at[e, peer], slot_in.at[e], slot_sem.at[e])
        slot_in[e, blk] = slot_out[e, blk]
        if follow is None:
            all_of(meta_all, meta_sem.at[1])
            follow = successor(
                meta_all[:, 0, :].astype(jnp.float32), meta_all[:, 1, :].astype(jnp.float32),
                blk, tiles, key_count)
        meanwhile()
        all_of(slot_in.at[e], slot_sem.at[e, 1])
        next_out[e] = pick(follow, slot_in[e].reshape(slots, rows)).reshape(n_blk, 2, rows)
        to_blk(lambda peer: next_out.at[e, peer], next_in.at[e], next_sem.at[e])
        next_in[e, blk] = next_out[e, blk]
        return follow

    def from_owners(e):
        all_of(next_in.at[e], next_sem.at[e, 1])
        there[...] = pick(from_slots, next_in[e].reshape(slots, rows))

    share_copies = to_src(lambda peer: shares.at[src], shares.at[src], share_sem)
    part_copies = to_src(
        lambda peer: vals.at[pl.ds(pl.multiple_of(peer * share, share), share)], parts.at[src], part_sem)

    @pl.when(src == leader)
    def _():
        pl.semaphore_wait(barrier, n_blk - 1)
        for step in src_steps:
            pl.semaphore_signal(open_sem, 1, device_id={"src": lax.rem(src + step, n_src)})

    @pl.when(src != leader)
    def _():
        pl.semaphore_wait(open_sem, 1)

    to_blk(lambda peer: meta_own, meta_all, meta_sem)
    for copy in share_copies:
        copy.wait()
    fixed[0] = functools.reduce(jnp.add, [shares[s, 0] for s in range(n_src)])
    fixed[1] = functools.reduce(jnp.add, [shares[s, 1] for s in range(n_src)])
    here[...] = fixed[0] / fixed[1]
    follow = through_owners(0, here[...], None)

    for copy in part_copies:
        copy.wait()

    @pl.loop(0, share)
    def _(k):
        full[src, k] = functools.reduce(jnp.add, [parts[s, k] for s in range(n_src)])

    first = pl.multiple_of(src * share, share)

    @pl.loop(0, share // 8)
    def _(g):
        near[pl.ds(pl.multiple_of(first + g * 8, 8), 8), :] = products(
            full.at[src], cols, here, g * 8, first + g * 8, 0)

    from_owners(0)
    for g in range(share // 8):
        at = pl.ds(pl.multiple_of(first + g * 8, 8), 8)
        total = near[at, :] + products(full.at[src], cols, there, g * 8, first + g * 8, rows)
        quarters[src, pl.ds(g * 8, 8), :] = (fixed[0, at, :] - total) / fixed[1, at, :]
    quarter_copies = to_src(lambda peer: quarters.at[src], quarters.at[src], quarter_sem)
    to_right, to_left = ring_copy(src, None, 1, 0), ring_copy(src, None, -1, 1)
    to_right.start()
    to_left.start()
    for copy in quarter_copies:
        copy.wait()
    here[...] = quarters[...].reshape(tiles, rows)

    left, right, across = (src - 1) % n_src, (src + 1) % n_src, (src + 2) % n_src
    halves = pl.ds(0, share // 2), pl.ds(share // 2, share // 2)
    onward = ring_copy(left, halves[0], 1, 2), ring_copy(right, halves[1], -1, 3)

    def pass_on():
        to_right.wait()
        onward[0].start()
        to_left.wait()
        onward[1].start()

    through_owners(1, here[...], follow, pass_on)

    def near_of(s):
        @pl.loop(0, share // 8)
        def _(g):
            start = s * share + g * 8
            near[pl.ds(pl.multiple_of(start, 8), 8), :] = products(full.at[s], cols, here, g * 8, start, 0)

    for chunk in (src, left, right):
        near_of(chunk)
    onward[0].wait()
    onward[1].wait()
    near_of(across)
    from_owners(1)
    for s in range(n_src):
        for g in range(share // 8):
            at = pl.ds(s * share + g * 8, 8)
            total = near[at, :] + products(full.at[s], cols, there, g * 8, s * share + g * 8, rows)
            out[at, :] = (fixed[0, at, :] - total) / fixed[1, at, :]

    all_of(meta_all, meta_sem.at[0])
    for e in range(SWEEPS - 1):
        all_of(slot_out.at[e], slot_sem.at[e, 0])
        all_of(next_out.at[e], next_sem.at[e, 0])


def solution(mesh):
    n_src, n_blk = mesh.shape["src"], mesh.shape["blk"]
    grid = (4, n_blk // 8)

    def on_device(values, diagonal, rhs_parts, owner_map, columns, destination, order_keys):
        tiles, stored, rows = columns.shape
        key_count = float(tiles * n_blk)
        row = jnp.float32
        anywhere = pl.BlockSpec(memory_space=pl.ANY)
        steps = SWEEPS - 1
        dma = pltpu.SemaphoreType.DMA
        return pl.pallas_call(
            functools.partial(kernel, n_src, n_blk, grid, tiles, stored, rows, key_count),
            out_shape=pltpu.VMEM((tiles, rows), row),
            in_specs=[anywhere] * 7,
            out_specs=pl.BlockSpec(memory_space=pltpu.VMEM),
            scratch_shapes=[
                pltpu.VMEM((tiles, stored, rows), row),
                pltpu.VMEM((tiles, stored, rows), jnp.int32),
                pltpu.VMEM((tiles, rows), row),
                pltpu.VMEM((tiles, rows), row),
                pltpu.VMEM((tiles, rows), jnp.int32),
                pltpu.VMEM((1, tiles), jnp.int32),
                pltpu.VMEM((1, tiles), jnp.int32),
                pltpu.VMEM((2, rows), jnp.int32),
                pltpu.VMEM((n_blk, 2, rows), jnp.int32),
                pltpu.VMEM((n_src, 2, tiles, rows), row),
                pltpu.VMEM((steps, n_blk, 2, rows), row),
                pltpu.VMEM((steps, n_blk, 2, rows), row),
                pltpu.VMEM((steps, n_blk, 2, rows), row),
                pltpu.VMEM((steps, n_blk, 2, rows), row),
                pltpu.VMEM((n_src, tiles // n_src, stored, rows), row),
                pltpu.VMEM((n_src, tiles // n_src, stored, rows), row),
                pltpu.VMEM((n_src, tiles // n_src, rows), row),
                pltpu.VMEM((tiles, rows), row),
                pltpu.VMEM((tiles, rows), row),
                pltpu.VMEM((tiles, rows), row),
                pltpu.VMEM((2, tiles, rows), row),
                dma((8,)),
                dma((2,)),
                dma((2, n_src)),
                dma((steps, 2)),
                dma((steps, 2)),
                dma((2, n_src)),
                dma((2, 4)),
                dma((2, n_src)),
                pltpu.SemaphoreType.REGULAR,
                pltpu.SemaphoreType.REGULAR,
            ],
            compiler_params=pltpu.CompilerParams(collective_id=0, has_side_effects=True),
            name="sweeps",
        )(values, columns, diagonal, rhs_parts, owner_map,
          destination.reshape(1, tiles), order_keys.reshape(1, tiles))

    placed = (
        P("src", "blk", None, None), P("src", "blk", None), P("src", "blk", None),
        P("blk", None), P("blk", None, None), P("blk", None), P("blk"),
    )
    return jax.shard_map(
        on_device, mesh=mesh, in_specs=placed, out_specs=P("blk", None), check_vma=False)
```

```python
import functools

import jax
import jax.numpy as jnp
from jax import lax
from jax.experimental import pallas as pl
from jax.experimental.pallas import tpu as pltpu
from jax.sharding import PartitionSpec as P

SWEEPS = 3
EXACT = lax.Precision.HIGHEST


def pick(selector, table):
    return jnp.dot(selector, table, precision=EXACT, preferred_element_type=jnp.float32)


def iota(shape, dim):
    return lax.broadcasted_iota(jnp.int32, shape, dim)


def turned(row, size):
    square = jnp.where(iota((size, size), 0) == iota((size, size), 1), row, 0.0)
    return jnp.sum(square, axis=1, keepdims=True)


def source_slots(owner_row, tiles, slots):
    owner_col = turned(owner_row, tiles)
    same = owner_col == owner_row
    row_at, col_at = iota((tiles, tiles), 0), iota((tiles, tiles), 1)
    before_col = jnp.sum(jnp.where(same & (col_at < row_at), 1.0, 0.0), axis=1, keepdims=True)
    before_row = jnp.sum(jnp.where(same & (row_at < col_at), 1.0, 0.0), axis=0, keepdims=True)
    slot_col = 2.0 * owner_col + before_col
    slot_row = 2.0 * owner_row + before_row
    to_slots = jnp.where(iota((slots, tiles), 0).astype(jnp.float32) == slot_row, 1.0, 0.0)
    from_slots = jnp.where(iota((tiles, slots), 1).astype(jnp.float32) == slot_col, 1.0, 0.0)
    return to_slots, from_slots


def successor(owners, keys, me, tiles, key_count):
    peers, width = owners.shape
    slots = 2 * peers
    lane = iota((peers, width), 1).astype(jnp.float32)
    mine = (owners == me.astype(jnp.float32)) & (lane < tiles)
    first = jnp.min(jnp.where(mine, lane, 1e6), axis=1, keepdims=True)
    last = jnp.max(jnp.where(mine, lane, -1.0), axis=1, keepdims=True)
    key_first = jnp.sum(jnp.where(mine & (lane == first), keys, 0.0), axis=1, keepdims=True)
    key_last = jnp.sum(jnp.where(mine & (lane == last), keys, 0.0), axis=1, keepdims=True)
    key_first = jnp.where(last >= 0.0, key_first, -1.0)
    key_last = jnp.where(last > first, key_last, -1.0)
    slot = iota((peers, slots), 1)
    chosen = jnp.where(slot % 2 == 1, key_last, key_first)
    key_row = jnp.sum(jnp.where(slot // 2 == iota((peers, slots), 0), chosen, 0.0), axis=0, keepdims=True)
    ahead = key_row - turned(key_row, slots) - 1.0
    ahead = jnp.where(ahead < 0.0, ahead + key_count, ahead)
    ahead = jnp.where(key_row >= 0.0, ahead, 4.0 * key_count)
    nearest = jnp.min(ahead, axis=1, keepdims=True)
    return jnp.where(ahead == nearest, 1.0, 0.0)


def folded(parts):
    parts = [parts[k] for k in (0, 4, 2, 6, 1, 5, 3, 7)]
    line = iota(parts[0].shape, 0)
    for step in (1, 2, 4):
        half = len(parts) // 2
        low = (line & step) == 0
        parts = [
            jnp.where(low, parts[k], parts[k + half])
            + pltpu.roll(jnp.where(low, parts[k + half], parts[k]), step, 0)
            for k in range(half)
        ]
    return parts[0]


def products(vals, cols, lines, v0, t0, bit):
    _, stored, rows = cols.shape
    parts = []
    for k in range(8):
        line = jnp.broadcast_to(lines[pl.ds(t0 + k, 1), :], (8, rows))
        total = None
        for j in range(stored // 8):
            code = cols[t0 + k, pl.ds(8 * j, 8), :]
            near = jnp.take_along_axis(line, code & (rows - 1), axis=1, mode="promise_in_bounds")
            term = jnp.where((code & rows) == bit, vals[v0 + k, pl.ds(8 * j, 8), :], 0.0) * near
            total = term if total is None else total + term
        parts.append(total)
    return folded(parts)


def kernel(
    n_src, n_blk, grid, tiles, stored, rows, key_count,
    vals_in, cols_in, diag_in, rhs_in, map_in, dest_in, keys_in, out,
    vals, cols, diag, rhs, owner_map, dest, keys,
    meta_own, meta_all, shares, slot_out, slot_in, next_out, next_in,
    hold, full, quarters, here, there, near, fixed,
    load_sem, meta_sem, share_sem, slot_sem, next_sem, part_sem, full_sem, quarter_sem, group_sem, open_sem,
):
    src, blk = lax.axis_index("src"), lax.axis_index("blk")
    slots = 2 * n_blk
    share = tiles // n_src
    n_y, n_z = grid
    y, z, core = blk // (2 * n_z), (blk // 2) % n_z, blk % 2
    src_steps = sorted(range(1, n_src), key=lambda step: -min(step, n_src - step))

    def by_distance(n):
        return sorted(range(n), key=lambda d: -min(d, n - d))

    at_z = {d: (z + d) % n_z * 2 for d in range(n_z)}
    at_y = {d: (y + d) % n_y * (2 * n_z) for d in range(n_y)}
    at_core = core, 1 - core
    others = [
        at_y[to_y] + at_z[to_z] + at_core[to_core]
        for to_z in by_distance(n_z) for to_y in by_distance(n_y) for to_core in (1, 0)
    ][:-1]

    barrier = pltpu.get_barrier_semaphore()
    hub, relay = 0, 1

    @pl.when(src != hub)
    def _():
        pl.semaphore_signal(barrier, 1, device_id={"src": hub})

    plane = jnp.maximum(src, relay)

    for peer in others:
        pl.semaphore_signal(barrier, 1, device_id={"src": plane, "blk": peer})

    loads = [
        pltpu.make_async_copy(a, b, load_sem.at[k])
        for k, (a, b) in enumerate((
            (dest_in, dest), (keys_in, keys), (map_in, owner_map), (rhs_in.at[0], rhs),
            (diag_in.at[0], diag), (vals_in.at[0], vals), (cols_in, cols)))
    ]
    for load in loads:
        load.start()
    loads[0].wait()
    loads[1].wait()
    meta_own[...] = jnp.zeros_like(meta_own)
    meta_own[0:1, 0:tiles] = dest[...]
    meta_own[1:2, 0:tiles] = keys[...]
    meta_all[blk] = meta_own[...]
    to_slots, from_slots = source_slots(dest[...].astype(jnp.float32), tiles, slots)
    for load in loads[2:5]:
        load.wait()
    shares[src, 0] = jnp.where(owner_map[...] == src, rhs[...], 0.0)
    shares[src, 1] = diag[...]
    for load in loads[5:]:
        load.wait()

    @pl.when(src == hub)
    def _():
        pl.semaphore_wait(barrier, n_src - 1)
        for peer in range(1, n_src):
            pl.semaphore_signal(group_sem, 1, device_id={"src": peer})

    @pl.when(src != hub)
    def _():
        pl.semaphore_wait(group_sem, 1)

    def to_src(source, target, sem):
        copies = []
        for step in src_steps:
            peer = lax.rem(src + step, n_src)
            copies.append(pltpu.make_async_remote_copy(
                src_ref=source(peer), dst_ref=target, send_sem=sem.at[0, step],
                recv_sem=sem.at[1, step], device_id={"src": peer}))
        for copy in copies:
            copy.start()
        return copies

    def to_blk(source, target, sem):
        for peer in others:
            pltpu.make_async_remote_copy(
                src_ref=source(peer), dst_ref=target.at[blk],
                send_sem=sem.at[0], recv_sem=sem.at[1], device_id={"blk": peer}).start()

    left, right, across = (src - 1) % n_src, (src + 1) % n_src, (src + 2) % n_src
    half = share // 2
    halves = pl.ds(0, half), pl.ds(half, half)

    def pass_copy(source, target, step, k):
        return pltpu.make_async_remote_copy(
            src_ref=source, dst_ref=target, send_sem=part_sem.at[0, k], recv_sem=part_sem.at[1, k],
            device_id={"src": (src + step) % n_src})

    def piece(chunk, h):
        return vals.at[pl.ds(pl.multiple_of(chunk * share + h * half, half), half)]

    scattered = (
        pass_copy(piece(across, 0), hold.at[0], 1, 0), pass_copy(piece(across, 1), hold.at[1], -1, 1),
        pass_copy(piece(right, 1), hold.at[2], 1, 2), pass_copy(piece(left, 0), hold.at[3], -1, 3))
    paired = pass_copy(hold.at[4], hold.at[6], 1, 4), pass_copy(hold.at[5], hold.at[7], -1, 5)

    def scatter():
        for copy in scattered:
            copy.start()

    def pair():
        for copy in scattered:
            copy.wait()

        @pl.loop(0, half)
        def _(k):
            hold[4, k] = vals[right * share + k] + hold[0, k]
            hold[5, k] = vals[left * share + half + k] + hold[1, k]

        for copy in paired:
            copy.start()

    def ring_copy(chunk, part, step, k):
        block = full.at[chunk, part] if part is not None else full.at[chunk]
        return pltpu.make_async_remote_copy(
            src_ref=block, dst_ref=block, send_sem=full_sem.at[0, k], recv_sem=full_sem.at[1, k],
            device_id={"src": (src + step) % n_src})

    def all_of(buffer, sem):
        most = buffer.at[pl.ds(0, n_blk - 1)]
        pltpu.make_async_copy(most, most, sem).wait()

    def through_owners(e, lines, follow, after_first, after_second):
        slot_out[e] = pick(to_slots, lines).reshape(n_blk, 2, rows)
        to_blk(lambda peer: slot_out.at[e, peer], slot_in.at[e], slot_sem.at[e])
        after_first()
        slot_in[e, blk] = slot_out[e, blk]
        if follow is None:
            all_of(meta_all, meta_sem.at[1])
            follow = successor(
                meta_all[:, 0, :].astype(jnp.float32), meta_all[:, 1, :].astype(jnp.float32),
                blk, tiles, key_count)
        all_of(slot_in.at[e], slot_sem.at[e, 1])
        next_out[e] = pick(follow, slot_in[e].reshape(slots, rows)).reshape(n_blk, 2, rows)
        to_blk(lambda peer: next_out.at[e, peer], next_in.at[e], next_sem.at[e])
        next_in[e, blk] = next_out[e, blk]
        after_second()
        return follow

    def from_owners(e):
        all_of(next_in.at[e], next_sem.at[e, 1])
        there[...] = pick(from_slots, next_in[e].reshape(slots, rows))

    share_copies = to_src(lambda peer: shares.at[src], shares.at[src], share_sem)
    @pl.when(src == hub)
    def _():
        pl.semaphore_wait(open_sem, 1)

    @pl.when(src == relay)
    def _():
        pl.semaphore_wait(barrier, 2 * (n_blk - 1))
        pl.semaphore_signal(open_sem, 1, device_id={"src": hub})

    @pl.when(src > relay)
    def _():
        pl.semaphore_wait(barrier, n_blk - 1)

    to_blk(lambda peer: meta_own, meta_all, meta_sem)
    for copy in share_copies:
        copy.wait()
    fixed[0] = functools.reduce(jnp.add, [shares[s, 0] for s in range(n_src)])
    fixed[1] = functools.reduce(jnp.add, [shares[s, 1] for s in range(n_src)])
    here[...] = fixed[0] / fixed[1]
    follow = through_owners(0, here[...], None, scatter, pair)

    for copy in paired:
        copy.wait()

    @pl.loop(0, half)
    def _(k):
        full[src, k] = vals[src * share + k] + hold[3, k] + hold[6, k]
        full[src, half + k] = vals[src * share + half + k] + hold[2, k] + hold[7, k]

    first = pl.multiple_of(src * share, share)

    @pl.loop(0, share // 8)
    def _(g):
        near[pl.ds(pl.multiple_of(first + g * 8, 8), 8), :] = products(
            full.at[src], cols, here, g * 8, first + g * 8, 0)

    from_owners(0)
    for g in range(share // 8):
        at = pl.ds(pl.multiple_of(first + g * 8, 8), 8)
        total = near[at, :] + products(full.at[src], cols, there, g * 8, first + g * 8, rows)
        quarters[src, pl.ds(g * 8, 8), :] = (fixed[0, at, :] - total) / fixed[1, at, :]
    quarter_copies = to_src(lambda peer: quarters.at[src], quarters.at[src], quarter_sem)
    for copy in quarter_copies:
        copy.wait()
    here[...] = quarters[...].reshape(tiles, rows)

    gathered = ring_copy(src, None, 1, 0), ring_copy(src, None, -1, 1)
    onward = ring_copy(left, halves[0], 1, 2), ring_copy(right, halves[1], -1, 3)

    def gather():
        for copy in gathered:
            copy.start()

    def pass_on():
        for copy in gathered:
            copy.wait()
        for copy in onward:
            copy.start()

    through_owners(1, here[...], follow, gather, pass_on)

    def near_of(s):
        @pl.loop(0, share // 8)
        def _(g):
            start = s * share + g * 8
            near[pl.ds(pl.multiple_of(start, 8), 8), :] = products(full.at[s], cols, here, g * 8, start, 0)

    for chunk in (src, left, right):
        near_of(chunk)
    onward[0].wait()
    onward[1].wait()
    near_of(across)
    from_owners(1)
    for s in range(n_src):
        for g in range(share // 8):
            at = pl.ds(s * share + g * 8, 8)
            total = near[at, :] + products(full.at[s], cols, there, g * 8, s * share + g * 8, rows)
            out[at, :] = (fixed[0, at, :] - total) / fixed[1, at, :]

    all_of(meta_all, meta_sem.at[0])
    for e in range(SWEEPS - 1):
        all_of(slot_out.at[e], slot_sem.at[e, 0])
        all_of(next_out.at[e], next_sem.at[e, 0])


def solution(mesh):
    n_src, n_blk = mesh.shape["src"], mesh.shape["blk"]
    grid = (4, n_blk // 8)

    def on_device(values, diagonal, rhs_parts, owner_map, columns, destination, order_keys):
        tiles, stored, rows = columns.shape
        key_count = float(tiles * n_blk)
        row = jnp.float32
        anywhere = pl.BlockSpec(memory_space=pl.ANY)
        steps = SWEEPS - 1
        dma = pltpu.SemaphoreType.DMA
        return pl.pallas_call(
            functools.partial(kernel, n_src, n_blk, grid, tiles, stored, rows, key_count),
            out_shape=pltpu.VMEM((tiles, rows), row),
            in_specs=[anywhere] * 7,
            out_specs=pl.BlockSpec(memory_space=pltpu.VMEM),
            scratch_shapes=[
                pltpu.VMEM((tiles, stored, rows), row),
                pltpu.VMEM((tiles, stored, rows), jnp.int32),
                pltpu.VMEM((tiles, rows), row),
                pltpu.VMEM((tiles, rows), row),
                pltpu.VMEM((tiles, rows), jnp.int32),
                pltpu.VMEM((1, tiles), jnp.int32),
                pltpu.VMEM((1, tiles), jnp.int32),
                pltpu.VMEM((2, rows), jnp.int32),
                pltpu.VMEM((n_blk, 2, rows), jnp.int32),
                pltpu.VMEM((n_src, 2, tiles, rows), row),
                pltpu.VMEM((steps, n_blk, 2, rows), row),
                pltpu.VMEM((steps, n_blk, 2, rows), row),
                pltpu.VMEM((steps, n_blk, 2, rows), row),
                pltpu.VMEM((steps, n_blk, 2, rows), row),
                pltpu.VMEM((8, tiles // n_src // 2, stored, rows), row),
                pltpu.VMEM((n_src, tiles // n_src, stored, rows), row),
                pltpu.VMEM((n_src, tiles // n_src, rows), row),
                pltpu.VMEM((tiles, rows), row),
                pltpu.VMEM((tiles, rows), row),
                pltpu.VMEM((tiles, rows), row),
                pltpu.VMEM((2, tiles, rows), row),
                dma((7,)),
                dma((2,)),
                dma((2, n_src)),
                dma((steps, 2)),
                dma((steps, 2)),
                dma((2, 6)),
                dma((2, 4)),
                dma((2, n_src)),
                pltpu.SemaphoreType.REGULAR,
                pltpu.SemaphoreType.REGULAR,
            ],
            compiler_params=pltpu.CompilerParams(collective_id=0, has_side_effects=True),
            name="sweeps",
        )(values, columns, diagonal, rhs_parts, owner_map,
          destination.reshape(1, tiles), order_keys.reshape(1, tiles))

    placed = (
        P("src", "blk", None, None), P("src", "blk", None), P("src", "blk", None),
        P("blk", None), P("blk", None, None), P("blk", None), P("blk"),
    )
    return jax.shard_map(
        on_device, mesh=mesh, in_specs=placed, out_specs=P("blk", None), check_vma=False)
```

```python
import functools

import jax
import jax.numpy as jnp
from jax import lax
from jax.experimental import pallas as pl
from jax.experimental.pallas import tpu as pltpu
from jax.sharding import PartitionSpec as P

SWEEPS = 3
EXACT = lax.Precision.HIGHEST


def pick(selector, table):
    return jnp.dot(selector, table, precision=EXACT, preferred_element_type=jnp.float32)


def iota(shape, dim):
    return lax.broadcasted_iota(jnp.int32, shape, dim)


def turned(row, size):
    square = jnp.where(iota((size, size), 0) == iota((size, size), 1), row, 0.0)
    return jnp.sum(square, axis=1, keepdims=True)


def source_slots(owner_row, tiles, slots):
    owner_col = turned(owner_row, tiles)
    same = owner_col == owner_row
    row_at, col_at = iota((tiles, tiles), 0), iota((tiles, tiles), 1)
    before_col = jnp.sum(jnp.where(same & (col_at < row_at), 1.0, 0.0), axis=1, keepdims=True)
    before_row = jnp.sum(jnp.where(same & (row_at < col_at), 1.0, 0.0), axis=0, keepdims=True)
    slot_col = 2.0 * owner_col + before_col
    slot_row = 2.0 * owner_row + before_row
    to_slots = jnp.where(iota((slots, tiles), 0).astype(jnp.float32) == slot_row, 1.0, 0.0)
    from_slots = jnp.where(iota((tiles, slots), 1).astype(jnp.float32) == slot_col, 1.0, 0.0)
    return to_slots, from_slots


def successor(owners, keys, me, tiles, key_count):
    peers, width = owners.shape
    slots = 2 * peers
    lane = iota((peers, width), 1).astype(jnp.float32)
    mine = (owners == me.astype(jnp.float32)) & (lane < tiles)
    first = jnp.min(jnp.where(mine, lane, 1e6), axis=1, keepdims=True)
    last = jnp.max(jnp.where(mine, lane, -1.0), axis=1, keepdims=True)
    key_first = jnp.sum(jnp.where(mine & (lane == first), keys, 0.0), axis=1, keepdims=True)
    key_last = jnp.sum(jnp.where(mine & (lane == last), keys, 0.0), axis=1, keepdims=True)
    key_first = jnp.where(last >= 0.0, key_first, -1.0)
    key_last = jnp.where(last > first, key_last, -1.0)
    slot = iota((peers, slots), 1)
    chosen = jnp.where(slot % 2 == 1, key_last, key_first)
    key_row = jnp.sum(jnp.where(slot // 2 == iota((peers, slots), 0), chosen, 0.0), axis=0, keepdims=True)
    ahead = key_row - turned(key_row, slots) - 1.0
    ahead = jnp.where(ahead < 0.0, ahead + key_count, ahead)
    ahead = jnp.where(key_row >= 0.0, ahead, 4.0 * key_count)
    nearest = jnp.min(ahead, axis=1, keepdims=True)
    return jnp.where(ahead == nearest, 1.0, 0.0)


def folded(parts):
    parts = [parts[k] for k in (0, 4, 2, 6, 1, 5, 3, 7)]
    line = iota(parts[0].shape, 0)
    for step in (1, 2, 4):
        half = len(parts) // 2
        low = (line & step) == 0
        parts = [
            jnp.where(low, parts[k], parts[k + half])
            + pltpu.roll(jnp.where(low, parts[k + half], parts[k]), step, 0)
            for k in range(half)
        ]
    return parts[0]


def products(vals, cols, lines, v0, t0, bit):
    _, stored, rows = cols.shape
    parts = []
    for k in range(8):
        line = jnp.broadcast_to(lines[pl.ds(t0 + k, 1), :], (8, rows))
        total = None
        for j in range(stored // 8):
            code = cols[t0 + k, pl.ds(8 * j, 8), :]
            near = jnp.take_along_axis(line, code & (rows - 1), axis=1, mode="promise_in_bounds")
            term = jnp.where((code & rows) == bit, vals[v0 + k, pl.ds(8 * j, 8), :], 0.0) * near
            total = term if total is None else total + term
        parts.append(total)
    return folded(parts)


def kernel(
    n_src, n_blk, grid, tiles, stored, rows, key_count,
    vals_in, cols_in, diag_in, rhs_in, map_in, dest_in, keys_in, out,
    vals, cols, diag, rhs, owner_map, dest, keys,
    meta_own, meta_all, shares, slot_out, slot_in, next_out, next_in,
    hold, full, quarters, here, there, near, fixed,
    load_sem, meta_sem, share_sem, slot_sem, next_sem, part_sem, full_sem, quarter_sem, group_sem, open_sem,
):
    src, blk = lax.axis_index("src"), lax.axis_index("blk")
    slots = 2 * n_blk
    share = tiles // n_src
    n_y, n_z = grid
    y, z, core = blk // (2 * n_z), (blk // 2) % n_z, blk % 2
    src_steps = sorted(range(1, n_src), key=lambda step: -min(step, n_src - step))

    def by_distance(n):
        return sorted(range(n), key=lambda d: -min(d, n - d))

    at_z = {d: (z + d) % n_z * 2 for d in range(n_z)}
    at_y = {d: (y + d) % n_y * (2 * n_z) for d in range(n_y)}
    at_core = core, 1 - core
    others = [
        at_y[to_y] + at_z[to_z] + at_core[to_core]
        for to_z in by_distance(n_z) for to_y in by_distance(n_y) for to_core in (1, 0)
    ][:-1]

    barrier = pltpu.get_barrier_semaphore()
    hub, relay = 0, 1

    @pl.when(src != hub)
    def _():
        pl.semaphore_signal(barrier, 1, device_id={"src": hub})

    plane = jnp.maximum(src, relay)

    for peer in others:
        pl.semaphore_signal(barrier, 1, device_id={"src": plane, "blk": peer})

    loads = [
        pltpu.make_async_copy(a, b, load_sem.at[k])
        for k, (a, b) in enumerate((
            (dest_in, dest), (keys_in, keys), (map_in, owner_map), (rhs_in.at[0], rhs),
            (diag_in.at[0], diag), (vals_in.at[0], vals), (cols_in, cols)))
    ]
    for load in loads:
        load.start()
    loads[0].wait()
    loads[1].wait()
    meta_own[...] = jnp.zeros_like(meta_own)
    meta_own[0:1, 0:tiles] = dest[...]
    meta_own[1:2, 0:tiles] = keys[...]
    meta_all[blk] = meta_own[...]
    to_slots, from_slots = source_slots(dest[...].astype(jnp.float32), tiles, slots)
    for load in loads[2:5]:
        load.wait()
    shares[src, 0] = jnp.where(owner_map[...] == src, rhs[...], 0.0)
    shares[src, 1] = diag[...]
    for load in loads[5:]:
        load.wait()

    @pl.when(src == hub)
    def _():
        pl.semaphore_wait(barrier, n_src - 1)
        for peer in range(1, n_src):
            pl.semaphore_signal(group_sem, 1, device_id={"src": peer})

    @pl.when(src != hub)
    def _():
        pl.semaphore_wait(group_sem, 1)

    def to_src(source, target, sem):
        copies = []
        for step in src_steps:
            peer = lax.rem(src + step, n_src)
            copies.append(pltpu.make_async_remote_copy(
                src_ref=source(peer), dst_ref=target, send_sem=sem.at[0, step],
                recv_sem=sem.at[1, step], device_id={"src": peer}))
        for copy in copies:
            copy.start()
        return copies

    def to_blk(source, target, sem):
        for peer in others:
            pltpu.make_async_remote_copy(
                src_ref=source(peer), dst_ref=target.at[blk],
                send_sem=sem.at[0], recv_sem=sem.at[1], device_id={"blk": peer}).start()

    left, right, across = (src - 1) % n_src, (src + 1) % n_src, (src + 2) % n_src
    half = share // 2
    halves = pl.ds(0, half), pl.ds(half, half)

    def pass_copy(source, target, step, k):
        return pltpu.make_async_remote_copy(
            src_ref=source, dst_ref=target, send_sem=part_sem.at[0, k], recv_sem=part_sem.at[1, k],
            device_id={"src": (src + step) % n_src})

    def piece(chunk, h):
        return vals.at[pl.ds(pl.multiple_of(chunk * share + h * half, half), half)]

    scattered = (
        pass_copy(piece(across, 0), hold.at[0], 1, 0), pass_copy(piece(across, 1), hold.at[1], -1, 1),
        pass_copy(piece(right, 1), hold.at[2], 1, 2), pass_copy(piece(left, 0), hold.at[3], -1, 3))
    paired = pass_copy(hold.at[4], hold.at[6], 1, 4), pass_copy(hold.at[5], hold.at[7], -1, 5)

    def pair():
        for copy in scattered[:2]:
            copy.wait()

        @pl.loop(0, half)
        def _(k):
            hold[4, k] = vals[right * share + k] + hold[0, k]
            hold[5, k] = vals[left * share + half + k] + hold[1, k]

        for copy in (*paired, *scattered[2:]):
            copy.start()

    def ring_copy(chunk, part, step, k):
        block = full.at[chunk, part] if part is not None else full.at[chunk]
        return pltpu.make_async_remote_copy(
            src_ref=block, dst_ref=block, send_sem=full_sem.at[0, k], recv_sem=full_sem.at[1, k],
            device_id={"src": (src + step) % n_src})

    def all_of(buffer, sem):
        most = buffer.at[pl.ds(0, n_blk - 1)]
        pltpu.make_async_copy(most, most, sem).wait()

    def through_owners(e, lines, follow, after_first, after_second):
        slot_out[e] = pick(to_slots, lines).reshape(n_blk, 2, rows)
        to_blk(lambda peer: slot_out.at[e, peer], slot_in.at[e], slot_sem.at[e])
        after_first()
        slot_in[e, blk] = slot_out[e, blk]
        if follow is None:
            all_of(meta_all, meta_sem.at[1])
            follow = successor(
                meta_all[:, 0, :].astype(jnp.float32), meta_all[:, 1, :].astype(jnp.float32),
                blk, tiles, key_count)
        all_of(slot_in.at[e], slot_sem.at[e, 1])
        next_out[e] = pick(follow, slot_in[e].reshape(slots, rows)).reshape(n_blk, 2, rows)
        to_blk(lambda peer: next_out.at[e, peer], next_in.at[e], next_sem.at[e])
        next_in[e, blk] = next_out[e, blk]
        after_second()
        return follow

    def from_owners(e):
        all_of(next_in.at[e], next_sem.at[e, 1])
        there[...] = pick(from_slots, next_in[e].reshape(slots, rows))

    share_copies = to_src(lambda peer: shares.at[src], shares.at[src], share_sem)
    @pl.when(src == hub)
    def _():
        pl.semaphore_wait(open_sem, 1)

    @pl.when(src == relay)
    def _():
        pl.semaphore_wait(barrier, 2 * (n_blk - 1))
        pl.semaphore_signal(open_sem, 1, device_id={"src": hub})

    @pl.when(src > relay)
    def _():
        pl.semaphore_wait(barrier, n_blk - 1)

    to_blk(lambda peer: meta_own, meta_all, meta_sem)
    for copy in share_copies:
        copy.wait()
    for copy in scattered[:2]:
        copy.start()
    fixed[0] = functools.reduce(jnp.add, [shares[s, 0] for s in range(n_src)])
    fixed[1] = functools.reduce(jnp.add, [shares[s, 1] for s in range(n_src)])
    here[...] = fixed[0] / fixed[1]
    follow = through_owners(0, here[...], None, pair, lambda: None)

    for copy in (*scattered[2:], *paired):
        copy.wait()

    @pl.loop(0, half)
    def _(k):
        full[src, k] = vals[src * share + k] + hold[3, k] + hold[6, k]
        full[src, half + k] = vals[src * share + half + k] + hold[2, k] + hold[7, k]

    first = pl.multiple_of(src * share, share)

    @pl.loop(0, share // 8)
    def _(g):
        near[pl.ds(pl.multiple_of(first + g * 8, 8), 8), :] = products(
            full.at[src], cols, here, g * 8, first + g * 8, 0)

    from_owners(0)
    for g in range(share // 8):
        at = pl.ds(pl.multiple_of(first + g * 8, 8), 8)
        total = near[at, :] + products(full.at[src], cols, there, g * 8, first + g * 8, rows)
        quarters[src, pl.ds(g * 8, 8), :] = (fixed[0, at, :] - total) / fixed[1, at, :]
    quarter_copies = to_src(lambda peer: quarters.at[src], quarters.at[src], quarter_sem)
    for copy in quarter_copies:
        copy.wait()
    here[...] = quarters[...].reshape(tiles, rows)

    gathered = ring_copy(src, None, 1, 0), ring_copy(src, None, -1, 1)
    onward = ring_copy(left, halves[0], 1, 2), ring_copy(right, halves[1], -1, 3)

    def gather():
        for copy in gathered:
            copy.start()

    def pass_on():
        for copy in gathered:
            copy.wait()
        for copy in onward:
            copy.start()

    through_owners(1, here[...], follow, gather, pass_on)

    def near_of(s):
        @pl.loop(0, share // 8)
        def _(g):
            start = s * share + g * 8
            near[pl.ds(pl.multiple_of(start, 8), 8), :] = products(full.at[s], cols, here, g * 8, start, 0)

    for chunk in (src, left, right):
        near_of(chunk)
    onward[0].wait()
    onward[1].wait()
    near_of(across)
    from_owners(1)
    for s in range(n_src):
        for g in range(share // 8):
            at = pl.ds(s * share + g * 8, 8)
            total = near[at, :] + products(full.at[s], cols, there, g * 8, s * share + g * 8, rows)
            out[at, :] = (fixed[0, at, :] - total) / fixed[1, at, :]

    all_of(meta_all, meta_sem.at[0])
    for e in range(SWEEPS - 1):
        all_of(slot_out.at[e], slot_sem.at[e, 0])
        all_of(next_out.at[e], next_sem.at[e, 0])


def solution(mesh):
    n_src, n_blk = mesh.shape["src"], mesh.shape["blk"]
    grid = (4, n_blk // 8)

    def on_device(values, diagonal, rhs_parts, owner_map, columns, destination, order_keys):
        tiles, stored, rows = columns.shape
        key_count = float(tiles * n_blk)
        row = jnp.float32
        anywhere = pl.BlockSpec(memory_space=pl.ANY)
        steps = SWEEPS - 1
        dma = pltpu.SemaphoreType.DMA
        return pl.pallas_call(
            functools.partial(kernel, n_src, n_blk, grid, tiles, stored, rows, key_count),
            out_shape=pltpu.VMEM((tiles, rows), row),
            in_specs=[anywhere] * 7,
            out_specs=pl.BlockSpec(memory_space=pltpu.VMEM),
            scratch_shapes=[
                pltpu.VMEM((tiles, stored, rows), row),
                pltpu.VMEM((tiles, stored, rows), jnp.int32),
                pltpu.VMEM((tiles, rows), row),
                pltpu.VMEM((tiles, rows), row),
                pltpu.VMEM((tiles, rows), jnp.int32),
                pltpu.VMEM((1, tiles), jnp.int32),
                pltpu.VMEM((1, tiles), jnp.int32),
                pltpu.VMEM((2, rows), jnp.int32),
                pltpu.VMEM((n_blk, 2, rows), jnp.int32),
                pltpu.VMEM((n_src, 2, tiles, rows), row),
                pltpu.VMEM((steps, n_blk, 2, rows), row),
                pltpu.VMEM((steps, n_blk, 2, rows), row),
                pltpu.VMEM((steps, n_blk, 2, rows), row),
                pltpu.VMEM((steps, n_blk, 2, rows), row),
                pltpu.VMEM((8, tiles // n_src // 2, stored, rows), row),
                pltpu.VMEM((n_src, tiles // n_src, stored, rows), row),
                pltpu.VMEM((n_src, tiles // n_src, rows), row),
                pltpu.VMEM((tiles, rows), row),
                pltpu.VMEM((tiles, rows), row),
                pltpu.VMEM((tiles, rows), row),
                pltpu.VMEM((2, tiles, rows), row),
                dma((7,)),
                dma((2,)),
                dma((2, n_src)),
                dma((steps, 2)),
                dma((steps, 2)),
                dma((2, 6)),
                dma((2, 4)),
                dma((2, n_src)),
                pltpu.SemaphoreType.REGULAR,
                pltpu.SemaphoreType.REGULAR,
            ],
            compiler_params=pltpu.CompilerParams(collective_id=0, has_side_effects=True),
            name="sweeps",
        )(values, columns, diagonal, rhs_parts, owner_map,
          destination.reshape(1, tiles), order_keys.reshape(1, tiles))

    placed = (
        P("src", "blk", None, None), P("src", "blk", None), P("src", "blk", None),
        P("blk", None), P("blk", None, None), P("blk", None), P("blk"),
    )
    return jax.shard_map(
        on_device, mesh=mesh, in_specs=placed, out_specs=P("blk", None), check_vma=False)
```

```python
import functools

import jax
import jax.numpy as jnp
from jax import lax
from jax.experimental import pallas as pl
from jax.experimental.pallas import tpu as pltpu
from jax.sharding import PartitionSpec as P

SWEEPS = 3
EXACT = lax.Precision.HIGHEST


def pick(selector, table):
    return jnp.dot(selector, table, precision=EXACT, preferred_element_type=jnp.float32)


def iota(shape, dim):
    return lax.broadcasted_iota(jnp.int32, shape, dim)


def turned(row, size):
    square = jnp.where(iota((size, size), 0) == iota((size, size), 1), row, 0.0)
    return jnp.sum(square, axis=1, keepdims=True)


def slot_numbers(owner_row, tiles, slots):
    row_at, col_at = iota((tiles, tiles), 0), iota((tiles, tiles), 1)
    owner_col = jnp.sum(jnp.where(row_at == col_at, owner_row, 0), axis=1, keepdims=True)
    earlier = (owner_col == owner_row) & (row_at < col_at)
    before = jnp.sum(jnp.where(earlier, 1, 0), axis=0, keepdims=True)
    return jnp.minimum(2 * owner_row + jnp.minimum(before, 1), slots - 1)


def source_slots(owner_row, tiles, slots):
    owner_col = turned(owner_row, tiles)
    same = owner_col == owner_row
    row_at, col_at = iota((tiles, tiles), 0), iota((tiles, tiles), 1)
    before_row = jnp.sum(jnp.where(same & (row_at < col_at), 1.0, 0.0), axis=0, keepdims=True)
    slot_row = 2.0 * owner_row + before_row
    to_slots = jnp.where(iota((slots, tiles), 0).astype(jnp.float32) == slot_row, 1.0, 0.0)
    return to_slots


def successor(owners, keys, me, tiles, key_count):
    peers, width = owners.shape
    slots = 2 * peers
    lane = iota((peers, width), 1).astype(jnp.float32)
    mine = (owners == me.astype(jnp.float32)) & (lane < tiles)
    first = jnp.min(jnp.where(mine, lane, 1e6), axis=1, keepdims=True)
    last = jnp.max(jnp.where(mine, lane, -1.0), axis=1, keepdims=True)
    key_first = jnp.sum(jnp.where(mine & (lane == first), keys, 0.0), axis=1, keepdims=True)
    key_last = jnp.sum(jnp.where(mine & (lane == last), keys, 0.0), axis=1, keepdims=True)
    key_first = jnp.where(last >= 0.0, key_first, -1.0)
    key_last = jnp.where(last > first, key_last, -1.0)
    slot = iota((peers, slots), 1)
    chosen = jnp.where(slot % 2 == 1, key_last, key_first)
    key_row = jnp.sum(jnp.where(slot // 2 == iota((peers, slots), 0), chosen, 0.0), axis=0, keepdims=True)
    ahead = key_row - turned(key_row, slots) - 1.0
    ahead = jnp.where(ahead < 0.0, ahead + key_count, ahead)
    ahead = jnp.where(key_row >= 0.0, ahead, 4.0 * key_count)
    nearest = jnp.min(ahead, axis=1, keepdims=True)
    return jnp.where(ahead == nearest, 1.0, 0.0)


def folded(parts):
    parts = [parts[k] for k in (0, 4, 2, 6, 1, 5, 3, 7)]
    line = iota(parts[0].shape, 0)
    for step in (1, 2, 4):
        half = len(parts) // 2
        low = (line & step) == 0
        parts = [
            jnp.where(low, parts[k], parts[k + half])
            + pltpu.roll(jnp.where(low, parts[k + half], parts[k]), step, 0)
            for k in range(half)
        ]
    return parts[0]


def products(vals, cols, line_of, v0, t0, bit):
    _, stored, rows = cols.shape
    parts = []
    for k in range(8):
        line = jnp.broadcast_to(line_of(t0 + k), (8, rows))
        total = None
        for j in range(stored // 8):
            code = cols[t0 + k, pl.ds(8 * j, 8), :]
            near = jnp.take_along_axis(line, code & (rows - 1), axis=1, mode="promise_in_bounds")
            term = jnp.where((code & rows) == bit, vals[v0 + k, pl.ds(8 * j, 8), :], 0.0) * near
            total = term if total is None else total + term
        parts.append(total)
    return folded(parts)


def kernel(
    n_src, n_blk, grid, tiles, stored, rows, key_count,
    vals_in, cols_in, diag_in, rhs_in, map_in, dest_in, keys_in, out,
    vals, cols, diag, rhs, owner_map, dest, keys,
    meta_own, meta_all, shares, slot_out, slot_in, next_out, next_in,
    hold, full, quarters, here, near, fixed, slot_row, slot_at,
    load_sem, meta_sem, share_sem, slot_sem, next_sem, part_sem, full_sem, quarter_sem, group_sem, open_sem, scalar_sem,
):
    src, blk = lax.axis_index("src"), lax.axis_index("blk")
    slots = 2 * n_blk
    share = tiles // n_src
    n_y, n_z = grid
    y, z, core = blk // (2 * n_z), (blk // 2) % n_z, blk % 2
    src_steps = sorted(range(1, n_src), key=lambda step: -min(step, n_src - step))

    def by_distance(n):
        return sorted(range(n), key=lambda d: -min(d, n - d))

    at_z = {d: (z + d) % n_z * 2 for d in range(n_z)}
    at_y = {d: (y + d) % n_y * (2 * n_z) for d in range(n_y)}
    at_core = core, 1 - core
    others = [
        at_y[to_y] + at_z[to_z] + at_core[to_core]
        for to_z in by_distance(n_z) for to_y in by_distance(n_y) for to_core in (1, 0)
    ][:-1]

    barrier = pltpu.get_barrier_semaphore()
    hub, relay = 0, 1

    @pl.when(src != hub)
    def _():
        pl.semaphore_signal(barrier, 1, device_id={"src": hub})

    plane = jnp.maximum(src, relay)

    for peer in others:
        pl.semaphore_signal(barrier, 1, device_id={"src": plane, "blk": peer})

    loads = [
        pltpu.make_async_copy(a, b, load_sem.at[k])
        for k, (a, b) in enumerate((
            (dest_in, dest), (keys_in, keys), (map_in, owner_map), (rhs_in.at[0], rhs),
            (diag_in.at[0], diag), (vals_in.at[0], vals), (cols_in, cols)))
    ]
    for load in loads:
        load.start()
    loads[0].wait()
    loads[1].wait()
    meta_own[...] = jnp.zeros_like(meta_own)
    meta_own[0:1, 0:tiles] = dest[...]
    meta_own[1:2, 0:tiles] = keys[...]
    meta_all[blk] = meta_own[...]
    slot_row[...] = slot_numbers(dest[...], tiles, slots)
    to_slots = source_slots(dest[...].astype(jnp.float32), tiles, slots)
    to_scalars = pltpu.make_async_copy(slot_row, slot_at, scalar_sem)
    to_scalars.start()
    for load in loads[2:5]:
        load.wait()
    shares[src, 0] = jnp.where(owner_map[...] == src, rhs[...], 0.0)
    shares[src, 1] = diag[...]
    for load in loads[5:]:
        load.wait()
    to_scalars.wait()

    @pl.when(src == hub)
    def _():
        pl.semaphore_wait(barrier, n_src - 1)
        for peer in range(1, n_src):
            pl.semaphore_signal(group_sem, 1, device_id={"src": peer})

    @pl.when(src != hub)
    def _():
        pl.semaphore_wait(group_sem, 1)

    def to_src(source, target, sem):
        copies = []
        for step in src_steps:
            peer = lax.rem(src + step, n_src)
            copies.append(pltpu.make_async_remote_copy(
                src_ref=source(peer), dst_ref=target, send_sem=sem.at[0, step],
                recv_sem=sem.at[1, step], device_id={"src": peer}))
        for copy in copies:
            copy.start()
        return copies

    def to_blk(source, target, sem):
        for peer in others:
            pltpu.make_async_remote_copy(
                src_ref=source(peer), dst_ref=target.at[blk],
                send_sem=sem.at[0], recv_sem=sem.at[1], device_id={"blk": peer}).start()

    left, right, across = (src - 1) % n_src, (src + 1) % n_src, (src + 2) % n_src
    half = share // 2
    halves = pl.ds(0, half), pl.ds(half, half)

    def pass_copy(source, target, step, k):
        return pltpu.make_async_remote_copy(
            src_ref=source, dst_ref=target, send_sem=part_sem.at[0, k], recv_sem=part_sem.at[1, k],
            device_id={"src": (src + step) % n_src})

    def piece(chunk, h):
        return vals.at[pl.ds(pl.multiple_of(chunk * share + h * half, half), half)]

    scattered = (
        pass_copy(piece(across, 0), hold.at[0], 1, 0), pass_copy(piece(across, 1), hold.at[1], -1, 1),
        pass_copy(piece(right, 1), hold.at[2], 1, 2), pass_copy(piece(left, 0), hold.at[3], -1, 3))
    paired = pass_copy(hold.at[4], hold.at[6], 1, 4), pass_copy(hold.at[5], hold.at[7], -1, 5)

    def pair():
        for copy in scattered[:2]:
            copy.wait()

        @pl.loop(0, half)
        def _(k):
            hold[4, k] = vals[right * share + k] + hold[0, k]
            hold[5, k] = vals[left * share + half + k] + hold[1, k]

        for copy in (*paired, *scattered[2:]):
            copy.start()

    def ring_copy(chunk, part, step, k):
        block = full.at[chunk, part] if part is not None else full.at[chunk]
        return pltpu.make_async_remote_copy(
            src_ref=block, dst_ref=block, send_sem=full_sem.at[0, k], recv_sem=full_sem.at[1, k],
            device_id={"src": (src + step) % n_src})

    def all_of(buffer, sem):
        most = buffer.at[pl.ds(0, n_blk - 1)]
        pltpu.make_async_copy(most, most, sem).wait()

    def through_owners(e, lines, follow, after_first, after_second):
        slot_out[e] = pick(to_slots, lines).reshape(n_blk, 2, rows)
        to_blk(lambda peer: slot_out.at[e, peer], slot_in.at[e], slot_sem.at[e])
        after_first()
        slot_in[e, blk] = slot_out[e, blk]
        if follow is None:
            all_of(meta_all, meta_sem.at[1])
            follow = successor(
                meta_all[:, 0, :].astype(jnp.float32), meta_all[:, 1, :].astype(jnp.float32),
                blk, tiles, key_count)
        all_of(slot_in.at[e], slot_sem.at[e, 1])
        next_out[e] = pick(follow, slot_in[e].reshape(slots, rows)).reshape(n_blk, 2, rows)
        to_blk(lambda peer: next_out.at[e, peer], next_in.at[e], next_sem.at[e])
        next_in[e, blk] = next_out[e, blk]
        after_second()
        return follow

    def own_line(tile):
        return here[pl.ds(tile, 1), :]

    def next_line(e):
        def line_of(tile):
            slot = slot_at[0, tile]
            return next_in[e, slot >> 1, pl.ds(slot & 1, 1), :]

        return line_of

    def from_owners(e):
        all_of(next_in.at[e], next_sem.at[e, 1])

    share_copies = to_src(lambda peer: shares.at[src], shares.at[src], share_sem)
    @pl.when(src == hub)
    def _():
        pl.semaphore_wait(open_sem, 1)

    @pl.when(src == relay)
    def _():
        pl.semaphore_wait(barrier, 2 * (n_blk - 1))
        pl.semaphore_signal(open_sem, 1, device_id={"src": hub})

    @pl.when(src > relay)
    def _():
        pl.semaphore_wait(barrier, n_blk - 1)

    to_blk(lambda peer: meta_own, meta_all, meta_sem)
    for copy in share_copies:
        copy.wait()
    for copy in scattered[:2]:
        copy.start()
    fixed[0] = functools.reduce(jnp.add, [shares[s, 0] for s in range(n_src)])
    fixed[1] = functools.reduce(jnp.add, [shares[s, 1] for s in range(n_src)])
    here[...] = fixed[0] / fixed[1]
    follow = through_owners(0, here[...], None, pair, lambda: None)

    for copy in (*scattered[2:], *paired):
        copy.wait()

    @pl.loop(0, half)
    def _(k):
        full[src, k] = vals[src * share + k] + hold[3, k] + hold[6, k]
        full[src, half + k] = vals[src * share + half + k] + hold[2, k] + hold[7, k]

    first = pl.multiple_of(src * share, share)

    @pl.loop(0, share // 8)
    def _(g):
        near[pl.ds(pl.multiple_of(first + g * 8, 8), 8), :] = products(
            full.at[src], cols, own_line, g * 8, first + g * 8, 0)

    from_owners(0)
    for g in range(share // 8):
        at = pl.ds(pl.multiple_of(first + g * 8, 8), 8)
        total = near[at, :] + products(full.at[src], cols, next_line(0), g * 8, first + g * 8, rows)
        quarters[src, pl.ds(g * 8, 8), :] = (fixed[0, at, :] - total) / fixed[1, at, :]
    quarter_copies = to_src(lambda peer: quarters.at[src], quarters.at[src], quarter_sem)
    for copy in quarter_copies:
        copy.wait()
    here[...] = quarters[...].reshape(tiles, rows)

    gathered = ring_copy(src, None, 1, 0), ring_copy(src, None, -1, 1)
    onward = ring_copy(left, halves[0], 1, 2), ring_copy(right, halves[1], -1, 3)

    def gather():
        for copy in gathered:
            copy.start()

    def pass_on():
        for copy in gathered:
            copy.wait()
        for copy in onward:
            copy.start()

    through_owners(1, here[...], follow, gather, pass_on)

    def near_of(s):
        @pl.loop(0, share // 8)
        def _(g):
            start = s * share + g * 8
            near[pl.ds(pl.multiple_of(start, 8), 8), :] = products(full.at[s], cols, own_line, g * 8, start, 0)

    for chunk in (src, left, right):
        near_of(chunk)
    onward[0].wait()
    onward[1].wait()
    near_of(across)
    from_owners(1)
    for s in range(n_src):
        for g in range(share // 8):
            at = pl.ds(s * share + g * 8, 8)
            total = near[at, :] + products(full.at[s], cols, next_line(1), g * 8, s * share + g * 8, rows)
            out[at, :] = (fixed[0, at, :] - total) / fixed[1, at, :]

    all_of(meta_all, meta_sem.at[0])
    for e in range(SWEEPS - 1):
        all_of(slot_out.at[e], slot_sem.at[e, 0])
        all_of(next_out.at[e], next_sem.at[e, 0])


def solution(mesh):
    n_src, n_blk = mesh.shape["src"], mesh.shape["blk"]
    grid = (4, n_blk // 8)

    def on_device(values, diagonal, rhs_parts, owner_map, columns, destination, order_keys):
        tiles, stored, rows = columns.shape
        key_count = float(tiles * n_blk)
        row = jnp.float32
        anywhere = pl.BlockSpec(memory_space=pl.ANY)
        steps = SWEEPS - 1
        dma = pltpu.SemaphoreType.DMA
        return pl.pallas_call(
            functools.partial(kernel, n_src, n_blk, grid, tiles, stored, rows, key_count),
            out_shape=pltpu.VMEM((tiles, rows), row),
            in_specs=[anywhere] * 7,
            out_specs=pl.BlockSpec(memory_space=pltpu.VMEM),
            scratch_shapes=[
                pltpu.VMEM((tiles, stored, rows), row),
                pltpu.VMEM((tiles, stored, rows), jnp.int32),
                pltpu.VMEM((tiles, rows), row),
                pltpu.VMEM((tiles, rows), row),
                pltpu.VMEM((tiles, rows), jnp.int32),
                pltpu.VMEM((1, tiles), jnp.int32),
                pltpu.VMEM((1, tiles), jnp.int32),
                pltpu.VMEM((2, rows), jnp.int32),
                pltpu.VMEM((n_blk, 2, rows), jnp.int32),
                pltpu.VMEM((n_src, 2, tiles, rows), row),
                pltpu.VMEM((steps, n_blk, 2, rows), row),
                pltpu.VMEM((steps, n_blk, 2, rows), row),
                pltpu.VMEM((steps, n_blk, 2, rows), row),
                pltpu.VMEM((steps, n_blk, 2, rows), row),
                pltpu.VMEM((8, tiles // n_src // 2, stored, rows), row),
                pltpu.VMEM((n_src, tiles // n_src, stored, rows), row),
                pltpu.VMEM((n_src, tiles // n_src, rows), row),
                pltpu.VMEM((tiles, rows), row),
                pltpu.VMEM((tiles, rows), row),
                pltpu.VMEM((2, tiles, rows), row),
                pltpu.VMEM((1, tiles), jnp.int32),
                pltpu.SMEM((1, tiles), jnp.int32),
                dma((7,)),
                dma((2,)),
                dma((2, n_src)),
                dma((steps, 2)),
                dma((steps, 2)),
                dma((2, 6)),
                dma((2, 4)),
                dma((2, n_src)),
                pltpu.SemaphoreType.REGULAR,
                pltpu.SemaphoreType.REGULAR,
                dma,
            ],
            compiler_params=pltpu.CompilerParams(collective_id=0, has_side_effects=True),
            name="sweeps",
        )(values, columns, diagonal, rhs_parts, owner_map,
          destination.reshape(1, tiles), order_keys.reshape(1, tiles))

    placed = (
        P("src", "blk", None, None), P("src", "blk", None), P("src", "blk", None),
        P("blk", None), P("blk", None, None), P("blk", None), P("blk"),
    )
    return jax.shard_map(
        on_device, mesh=mesh, in_specs=placed, out_specs=P("blk", None), check_vma=False)
```

```python
import functools

import jax
import jax.numpy as jnp
from jax import lax
from jax.experimental import pallas as pl
from jax.experimental.pallas import tpu as pltpu
from jax.sharding import PartitionSpec as P

SWEEPS = 3
EXACT = lax.Precision.HIGHEST


def pick(selector, table):
    return jnp.dot(selector, table, precision=EXACT, preferred_element_type=jnp.float32)


def iota(shape, dim):
    return lax.broadcasted_iota(jnp.int32, shape, dim)


def turned(row, size):
    square = jnp.where(iota((size, size), 0) == iota((size, size), 1), row, 0.0)
    return jnp.sum(square, axis=1, keepdims=True)


def slot_numbers(owner_row, tiles, slots):
    row_at, col_at = iota((tiles, tiles), 0), iota((tiles, tiles), 1)
    owner_col = jnp.sum(jnp.where(row_at == col_at, owner_row, 0), axis=1, keepdims=True)
    earlier = (owner_col == owner_row) & (row_at < col_at)
    before = jnp.sum(jnp.where(earlier, 1, 0), axis=0, keepdims=True)
    return jnp.minimum(2 * owner_row + jnp.minimum(before, 1), slots - 1)


def source_slots(owner_row, tiles, slots):
    owner_col = turned(owner_row, tiles)
    same = owner_col == owner_row
    row_at, col_at = iota((tiles, tiles), 0), iota((tiles, tiles), 1)
    before_row = jnp.sum(jnp.where(same & (row_at < col_at), 1.0, 0.0), axis=0, keepdims=True)
    slot_row = 2.0 * owner_row + before_row
    to_slots = jnp.where(iota((slots, tiles), 0).astype(jnp.float32) == slot_row, 1.0, 0.0)
    return to_slots


def successor(owners, keys, me, tiles, key_count):
    peers, width = owners.shape
    slots = 2 * peers
    lane = iota((peers, width), 1).astype(jnp.float32)
    mine = (owners == me.astype(jnp.float32)) & (lane < tiles)
    first = jnp.min(jnp.where(mine, lane, 1e6), axis=1, keepdims=True)
    last = jnp.max(jnp.where(mine, lane, -1.0), axis=1, keepdims=True)
    key_first = jnp.sum(jnp.where(mine & (lane == first), keys, 0.0), axis=1, keepdims=True)
    key_last = jnp.sum(jnp.where(mine & (lane == last), keys, 0.0), axis=1, keepdims=True)
    key_first = jnp.where(last >= 0.0, key_first, -1.0)
    key_last = jnp.where(last > first, key_last, -1.0)
    slot = iota((peers, slots), 1)
    chosen = jnp.where(slot % 2 == 1, key_last, key_first)
    key_row = jnp.sum(jnp.where(slot // 2 == iota((peers, slots), 0), chosen, 0.0), axis=0, keepdims=True)
    ahead = key_row - turned(key_row, slots) - 1.0
    ahead = jnp.where(ahead < 0.0, ahead + key_count, ahead)
    ahead = jnp.where(key_row >= 0.0, ahead, 4.0 * key_count)
    nearest = jnp.min(ahead, axis=1, keepdims=True)
    return jnp.where(ahead == nearest, 1.0, 0.0)


def folded(parts):
    parts = [parts[k] for k in (0, 4, 2, 6, 1, 5, 3, 7)]
    line = iota(parts[0].shape, 0)
    for step in (1, 2, 4):
        half = len(parts) // 2
        low = (line & step) == 0
        parts = [
            jnp.where(low, parts[k], parts[k + half])
            + pltpu.roll(jnp.where(low, parts[k + half], parts[k]), step, 0)
            for k in range(half)
        ]
    return parts[0]


def products(vals, cols, line_of, v0, t0, bit):
    _, stored, rows = cols.shape
    parts = []
    for k in range(8):
        line = jnp.broadcast_to(line_of(t0 + k), (8, rows))
        total = None
        for j in range(stored // 8):
            code = cols[t0 + k, pl.ds(8 * j, 8), :]
            near = jnp.take_along_axis(line, code & (rows - 1), axis=1, mode="promise_in_bounds")
            value = vals[v0 + k, pl.ds(8 * j, 8), :]
            term = (value if bit is None else jnp.where((code & rows) == bit, value, 0.0)) * near
            total = term if total is None else total + term
        parts.append(total)
    return folded(parts)


def kernel(
    n_src, n_blk, grid, tiles, stored, rows, key_count,
    vals_in, cols_in, diag_in, rhs_in, map_in, dest_in, keys_in, out,
    vals, cols, diag, rhs, owner_map, dest, keys,
    meta_own, meta_all, shares, slot_out, slot_in, next_out, next_in,
    hold, full, quarters, here, near, fixed, slot_row, slot_at,
    load_sem, meta_sem, share_sem, slot_sem, next_sem, part_sem, full_sem, quarter_sem, group_sem, open_sem, scalar_sem,
):
    src, blk = lax.axis_index("src"), lax.axis_index("blk")
    slots = 2 * n_blk
    share = tiles // n_src
    n_y, n_z = grid
    y, z, core = blk // (2 * n_z), (blk // 2) % n_z, blk % 2
    src_steps = sorted(range(1, n_src), key=lambda step: -min(step, n_src - step))

    def by_distance(n):
        return sorted(range(n), key=lambda d: -min(d, n - d))

    at_z = {d: (z + d) % n_z * 2 for d in range(n_z)}
    at_y = {d: (y + d) % n_y * (2 * n_z) for d in range(n_y)}
    at_core = core, 1 - core
    others = [
        at_y[to_y] + at_z[to_z] + at_core[to_core]
        for to_z in by_distance(n_z) for to_y in by_distance(n_y) for to_core in (1, 0)
    ][:-1]

    barrier = pltpu.get_barrier_semaphore()
    hub, relay = 0, 1

    @pl.when(src != hub)
    def _():
        pl.semaphore_signal(barrier, 1, device_id={"src": hub})

    plane = jnp.maximum(src, relay)

    for peer in others:
        pl.semaphore_signal(barrier, 1, device_id={"src": plane, "blk": peer})

    loads = [
        pltpu.make_async_copy(a, b, load_sem.at[k])
        for k, (a, b) in enumerate((
            (dest_in, dest), (keys_in, keys), (map_in, owner_map), (rhs_in.at[0], rhs),
            (diag_in.at[0], diag), (vals_in.at[0], vals), (cols_in, cols)))
    ]
    for load in loads:
        load.start()
    loads[0].wait()
    loads[1].wait()
    meta_own[...] = jnp.zeros_like(meta_own)
    meta_own[0:1, 0:tiles] = dest[...]
    meta_own[1:2, 0:tiles] = keys[...]
    meta_all[blk] = meta_own[...]
    slot_row[...] = slot_numbers(dest[...], tiles, slots)
    to_slots = source_slots(dest[...].astype(jnp.float32), tiles, slots)
    to_scalars = pltpu.make_async_copy(slot_row, slot_at, scalar_sem)
    to_scalars.start()
    for load in loads[2:5]:
        load.wait()
    shares[src, 0] = jnp.where(owner_map[...] == src, rhs[...], 0.0)
    shares[src, 1] = diag[...]
    for load in loads[5:]:
        load.wait()
    to_scalars.wait()

    @pl.when(src == hub)
    def _():
        pl.semaphore_wait(barrier, n_src - 1)
        for peer in range(1, n_src):
            pl.semaphore_signal(group_sem, 1, device_id={"src": peer})

    @pl.when(src != hub)
    def _():
        pl.semaphore_wait(group_sem, 1)

    def to_src(source, target, sem):
        copies = []
        for step in src_steps:
            peer = lax.rem(src + step, n_src)
            copies.append(pltpu.make_async_remote_copy(
                src_ref=source(peer), dst_ref=target, send_sem=sem.at[0, step],
                recv_sem=sem.at[1, step], device_id={"src": peer}))
        for copy in copies:
            copy.start()
        return copies

    def to_blk(source, target, sem):
        for peer in others:
            pltpu.make_async_remote_copy(
                src_ref=source(peer), dst_ref=target.at[blk],
                send_sem=sem.at[0], recv_sem=sem.at[1], device_id={"blk": peer}).start()

    left, right, across = (src - 1) % n_src, (src + 1) % n_src, (src + 2) % n_src
    half = share // 2
    halves = pl.ds(0, half), pl.ds(half, half)

    def pass_copy(source, target, step, k):
        return pltpu.make_async_remote_copy(
            src_ref=source, dst_ref=target, send_sem=part_sem.at[0, k], recv_sem=part_sem.at[1, k],
            device_id={"src": (src + step) % n_src})

    def piece(chunk, h):
        return vals.at[pl.ds(pl.multiple_of(chunk * share + h * half, half), half)]

    scattered = (
        pass_copy(piece(across, 0), hold.at[0], 1, 0), pass_copy(piece(across, 1), hold.at[1], -1, 1),
        pass_copy(piece(right, 1), hold.at[2], 1, 2), pass_copy(piece(left, 0), hold.at[3], -1, 3))
    paired = pass_copy(hold.at[4], hold.at[6], 1, 4), pass_copy(hold.at[5], hold.at[7], -1, 5)

    def pair():
        for copy in scattered[:2]:
            copy.wait()

        @pl.loop(0, half)
        def _(k):
            hold[4, k] = vals[right * share + k] + hold[0, k]
            hold[5, k] = vals[left * share + half + k] + hold[1, k]

        for copy in (*paired, *scattered[2:]):
            copy.start()

    def ring_copy(chunk, part, step, k):
        block = full.at[chunk, part] if part is not None else full.at[chunk]
        return pltpu.make_async_remote_copy(
            src_ref=block, dst_ref=block, send_sem=full_sem.at[0, k], recv_sem=full_sem.at[1, k],
            device_id={"src": (src + step) % n_src})

    def all_of(buffer, sem):
        most = buffer.at[pl.ds(0, n_blk - 1)]
        pltpu.make_async_copy(most, most, sem).wait()

    def through_owners(e, lines, follow, after_first, after_second):
        slot_out[e] = pick(to_slots, lines).reshape(n_blk, 2, rows)
        to_blk(lambda peer: slot_out.at[e, peer], slot_in.at[e], slot_sem.at[e])
        after_first()
        slot_in[e, blk] = slot_out[e, blk]
        if follow is None:
            all_of(meta_all, meta_sem.at[1])
            follow = successor(
                meta_all[:, 0, :].astype(jnp.float32), meta_all[:, 1, :].astype(jnp.float32),
                blk, tiles, key_count)
        all_of(slot_in.at[e], slot_sem.at[e, 1])
        next_out[e] = pick(follow, slot_in[e].reshape(slots, rows)).reshape(n_blk, 2, rows)
        to_blk(lambda peer: next_out.at[e, peer], next_in.at[e], next_sem.at[e])
        next_in[e, blk] = next_out[e, blk]
        after_second()
        return follow

    def own_line(tile):
        return here[pl.ds(tile, 1), :]

    def next_line(e):
        def line_of(tile):
            slot = slot_at[0, tile]
            return next_in[e, slot >> 1, pl.ds(slot & 1, 1), :]

        return line_of

    def from_owners(e):
        all_of(next_in.at[e], next_sem.at[e, 1])

    share_copies = to_src(lambda peer: shares.at[src], shares.at[src], share_sem)
    @pl.when(src == hub)
    def _():
        pl.semaphore_wait(open_sem, 1)

    @pl.when(src == relay)
    def _():
        pl.semaphore_wait(barrier, 2 * (n_blk - 1))
        pl.semaphore_signal(open_sem, 1, device_id={"src": hub})

    @pl.when(src > relay)
    def _():
        pl.semaphore_wait(barrier, n_blk - 1)

    to_blk(lambda peer: meta_own, meta_all, meta_sem)
    for copy in share_copies:
        copy.wait()
    for copy in scattered[:2]:
        copy.start()
    fixed[0] = functools.reduce(jnp.add, [shares[s, 0] for s in range(n_src)])
    fixed[1] = functools.reduce(jnp.add, [shares[s, 1] for s in range(n_src)])
    here[...] = fixed[0] / fixed[1]
    follow = through_owners(0, here[...], None, pair, lambda: None)

    for copy in (*scattered[2:], *paired):
        copy.wait()

    @pl.loop(0, half)
    def _(k):
        full[src, k] = vals[src * share + k] + hold[3, k] + hold[6, k]
        full[src, half + k] = vals[src * share + half + k] + hold[2, k] + hold[7, k]

    first = pl.multiple_of(src * share, share)

    @pl.loop(0, share // 8)
    def _(g):
        near[pl.ds(pl.multiple_of(first + g * 8, 8), 8), :] = products(
            full.at[src], cols, own_line, g * 8, first + g * 8, 0)

    from_owners(0)
    for g in range(share // 8):
        at = pl.ds(pl.multiple_of(first + g * 8, 8), 8)
        total = near[at, :] + products(full.at[src], cols, next_line(0), g * 8, first + g * 8, rows)
        quarters[src, pl.ds(g * 8, 8), :] = (fixed[0, at, :] - total) / fixed[1, at, :]
    quarter_copies = to_src(lambda peer: quarters.at[src], quarters.at[src], quarter_sem)
    for copy in quarter_copies:
        copy.wait()
    here[...] = quarters[...].reshape(tiles, rows)

    gathered = ring_copy(src, None, 1, 0), ring_copy(src, None, -1, 1)
    onward = ring_copy(left, halves[0], 1, 2), ring_copy(right, halves[1], -1, 3)

    def gather():
        for copy in gathered:
            copy.start()

    def pass_on():
        for copy in gathered:
            copy.wait()
        for copy in onward:
            copy.start()

    through_owners(1, here[...], follow, gather, pass_on)

    def near_of(s):
        @pl.loop(0, share // 8)
        def _(g):
            start = s * share + g * 8
            near[pl.ds(pl.multiple_of(start, 8), 8), :] = products(full.at[s], cols, own_line, g * 8, start, 0)
            for k in range(8):
                vals[start + k] = jnp.where((cols[start + k] & rows) == rows, full[s, g * 8 + k], 0.0)

    for chunk in (src, left, right):
        near_of(chunk)
    onward[0].wait()
    onward[1].wait()
    near_of(across)
    from_owners(1)
    for s in range(n_src):
        for g in range(share // 8):
            at = pl.ds(s * share + g * 8, 8)
            total = near[at, :] + products(vals, cols, next_line(1), s * share + g * 8, s * share + g * 8, None)
            out[at, :] = (fixed[0, at, :] - total) / fixed[1, at, :]

    all_of(meta_all, meta_sem.at[0])
    for e in range(SWEEPS - 1):
        all_of(slot_out.at[e], slot_sem.at[e, 0])
        all_of(next_out.at[e], next_sem.at[e, 0])


def solution(mesh):
    n_src, n_blk = mesh.shape["src"], mesh.shape["blk"]
    grid = (4, n_blk // 8)

    def on_device(values, diagonal, rhs_parts, owner_map, columns, destination, order_keys):
        tiles, stored, rows = columns.shape
        key_count = float(tiles * n_blk)
        row = jnp.float32
        anywhere = pl.BlockSpec(memory_space=pl.ANY)
        steps = SWEEPS - 1
        dma = pltpu.SemaphoreType.DMA
        return pl.pallas_call(
            functools.partial(kernel, n_src, n_blk, grid, tiles, stored, rows, key_count),
            out_shape=pltpu.VMEM((tiles, rows), row),
            in_specs=[anywhere] * 7,
            out_specs=pl.BlockSpec(memory_space=pltpu.VMEM),
            scratch_shapes=[
                pltpu.VMEM((tiles, stored, rows), row),
                pltpu.VMEM((tiles, stored, rows), jnp.int32),
                pltpu.VMEM((tiles, rows), row),
                pltpu.VMEM((tiles, rows), row),
                pltpu.VMEM((tiles, rows), jnp.int32),
                pltpu.VMEM((1, tiles), jnp.int32),
                pltpu.VMEM((1, tiles), jnp.int32),
                pltpu.VMEM((2, rows), jnp.int32),
                pltpu.VMEM((n_blk, 2, rows), jnp.int32),
                pltpu.VMEM((n_src, 2, tiles, rows), row),
                pltpu.VMEM((steps, n_blk, 2, rows), row),
                pltpu.VMEM((steps, n_blk, 2, rows), row),
                pltpu.VMEM((steps, n_blk, 2, rows), row),
                pltpu.VMEM((steps, n_blk, 2, rows), row),
                pltpu.VMEM((8, tiles // n_src // 2, stored, rows), row),
                pltpu.VMEM((n_src, tiles // n_src, stored, rows), row),
                pltpu.VMEM((n_src, tiles // n_src, rows), row),
                pltpu.VMEM((tiles, rows), row),
                pltpu.VMEM((tiles, rows), row),
                pltpu.VMEM((2, tiles, rows), row),
                pltpu.VMEM((1, tiles), jnp.int32),
                pltpu.SMEM((1, tiles), jnp.int32),
                dma((7,)),
                dma((2,)),
                dma((2, n_src)),
                dma((steps, 2)),
                dma((steps, 2)),
                dma((2, 6)),
                dma((2, 4)),
                dma((2, n_src)),
                pltpu.SemaphoreType.REGULAR,
                pltpu.SemaphoreType.REGULAR,
                dma,
            ],
            compiler_params=pltpu.CompilerParams(collective_id=0, has_side_effects=True),
            name="sweeps",
        )(values, columns, diagonal, rhs_parts, owner_map,
          destination.reshape(1, tiles), order_keys.reshape(1, tiles))

    placed = (
        P("src", "blk", None, None), P("src", "blk", None), P("src", "blk", None),
        P("blk", None), P("blk", None, None), P("blk", None), P("blk"),
    )
    return jax.shard_map(
        on_device, mesh=mesh, in_specs=placed, out_specs=P("blk", None), check_vma=False)
```
